32 devices in a mesh: band: 4 (over z), ga: 8 (over y, x, core).
Axes of the slice: x: 2, y: 2, z: 4, core: 2. Of those that a mesh axis runs over, the one named last changes fastest.
Arguments:
- waves: bfloat16 [2, 128, 8192], P(None, 'band', 'ga'), may hold values from -6 to 6
- occupations: float32 [128], P('band'), may hold values from 0.0015625 to 0.03125
- beta_table: float32 [72, 8192], P(None, 'ga'), may hold values from -0.046875 to 0.046875
- wave_miller: int32 [3, 8192], P(None, 'ga'), may hold values from 0 to 223
- atom_kinds: int32 [256], replicated, may hold values from 0 to 3
- atom_sites: int32 [3, 256], replicated, may hold values from 0 to 223
- aug_table: bfloat16 [684, 57344], P(None, ('band', 'ga')), may hold values from -0.00061035156 to 0.00061035156
- stick_columns: int32 [256], P(('band', 'ga')), may hold values from -1 to 14399, as said below
Outputs:
- density: float32 [2, 224, 240, 240], P(None, 'ga', 'band')
The draws below stay inside these ranges and needn't reach their ends.
Inputs may be any that keep to these rules, and one draw needn't show every extreme that they name: `stick_columns`: entry t is a slot of the device at place t // 8 in band-major order, of band index t // 64. -1 marks an empty slot; otherwise the entry c names the column x = (t // 64) * 60 + c // 240, y = c mod 240. Live columns of one band index are distinct. On each device the live slots come first and at least one is live; in each band index some device has all 8 slots live.
All inputs are finite; a program needn't handle non-finite values.
Results may differ from the reference program's by a relative error of at most 0.0035.
Values sent between devices are 32-bit elements; how exact they have to be, the bound alone decides.
A program may use at most 64 MiB of HBM per device.

```python
import math
import jax
import jax.numpy as jnp
import numpy as np
from jax import lax

NX = 240
NY = 240
NZ = 224
NH = 18
PAIRS = 171
SPECIES = 4
ATOMS = 256
BANDS = 128
GW = 8192
STK = 8
STICKS = 256
BLOCK_STICKS = 64
NXB = 60


def draw_stick_columns(key, part):
    groups = STICKS // BLOCK_STICKS
    devices = BLOCK_STICKS // STK
    group_keys = jax.random.split(jax.random.fold_in(key, 11), groups)

    def one_group(group_key):
        perm_key, count_key, full_key = jax.random.split(group_key, 3)
        chosen = jax.random.permutation(perm_key, NXB * NY)[:BLOCK_STICKS].astype(jnp.int32).reshape(devices, STK)
        live_count = jax.random.randint(count_key, (devices,), 1, STK // 2 + 1)
        fullest = jax.random.randint(full_key, (), 0, devices)
        live_count = jnp.where(jnp.arange(devices) == fullest, STK, live_count)
        slot_index = jnp.arange(STK)[None, :]
        return jnp.where(slot_index < live_count[:, None], chosen, -1).reshape(-1)
    return jax.vmap(one_group)(group_keys).reshape(-1).astype(jnp.int32)


def place_ends(values, own_key, least, high):
    longest = values.shape.index(max(values.shape))
    spots = []
    for shift in (0, 1):
        where = [jax.random.randint(jax.random.fold_in(own_key, axis), (), 0, length) for axis, length in enumerate(values.shape)]
        where[longest] = (where[longest] + shift) % values.shape[longest]
        spots.append(tuple(where))
    return values.at[spots[0]].set(least).at[spots[1]].set(high)


def levels(stream_key, extent, shards, low, top_value):
    level = 1.0
    for position, parts in shards:
        heights = jax.random.uniform(jax.random.fold_in(jax.random.fold_in(stream_key, 6), position), (parts,), jnp.float32, low / len(shards), top_value / len(shards))
        level = level * jnp.repeat(jnp.exp(heights), extent[position] // parts).reshape((-1,) + (1,) * (len(extent) - 1 - position))
    return level


def centred(key, extent, spread, limit, cuts=(), held_as=jnp.bfloat16):
    values = jax.random.normal(key, extent, jnp.float32) * spread
    if len(cuts) > 0:
        values = levels(key, extent, cuts, -0.22, 0.18) * values
    return jnp.clip(values, min=-limit, max=limit).astype(held_as)


def setup_inputs(seed: int = 0) -> dict:
    key_of = jax.random.split(jax.random.key(seed), 9)
    return {
        "waves": centred(key_of[0], (2, BANDS, GW), 1.0, 6.0, ((1, 4), (2, 8))),
        "occupations": jnp.clip(jnp.exp(math.log(0.03125) - 2.9957323 * jax.random.uniform(key_of[1], (BANDS,), jnp.float32) ** levels(key_of[1], (BANDS,), ((0, 4),), -0.2, 0.2)), 0.0015625, 0.03125),
        "beta_table": centred(key_of[2], (SPECIES * NH, GW), (2 * GW) ** -0.5, 0.046875, ((1, 8),), jnp.float32),
        "wave_miller": place_ends(jax.random.randint(key_of[3], (3, GW), 0, min(NX, min(NY, NZ))), jax.random.fold_in(key_of[3], 1), 0, (min(NX, min(NY, NZ))) - 1).astype(jnp.int32),
        "atom_kinds": place_ends(jax.random.randint(key_of[4], (ATOMS,), 0, SPECIES), jax.random.fold_in(key_of[4], 1), 0, SPECIES - 1).astype(jnp.int32),
        "atom_sites": place_ends(jax.random.randint(key_of[5], (3, ATOMS), 0, min(NX, min(NY, NZ))), jax.random.fold_in(key_of[5], 1), 0, (min(NX, min(NY, NZ))) - 1).astype(jnp.int32),
        "aug_table": centred(key_of[6], (SPECIES * PAIRS, STICKS * NZ), ((40.0 * ATOMS * STICKS * NZ) ** -0.5), 0.00061035156, ((1, 32),)),
        "stick_columns": draw_stick_columns(jax.random.fold_in(key_of[8], 71), 0),
    }


highest = lax.Precision.HIGHEST


def pair_tables(proj_count):
    ell_values = np.array([0, 0] + [1] * 6 + [2] * 10)
    pair_first, pair_second = np.triu_indices(proj_count)
    factors = np.where(pair_first == pair_second, 1.0, 2.0).astype(np.float32)
    parity = ((ell_values[pair_first] + ell_values[pair_second]) % 2).astype(np.float32)
    return pair_first * proj_count + pair_second, factors, parity


def phase_coefficients():
    ell_values = np.array([0, 0] + [1] * 6 + [2] * 10)
    coef_real = np.array([1.0, 0.0, -1.0])[ell_values]
    coef_imag = np.array([0.0, -1.0, 0.0])[ell_values]
    return jnp.asarray(coef_real, jnp.float32), jnp.asarray(coef_imag, jnp.float32)


def phase_angle(site_block, first, second, third):
    turn_count = ((site_block[0][:, None] * first[None, :]) % NX) * (NY * NZ)
    turn_count = turn_count + ((site_block[1][:, None] * second[None, :]) % NY) * (NX * NZ)
    turn_count = turn_count + ((site_block[2][:, None] * third[None, :]) % NZ) * (NX * NY)
    turn_count = (turn_count % (NX * NY * NZ)).astype(jnp.int32)
    angle_value = turn_count.astype(jnp.float32) * (2.0 * np.pi / (NX * NY * NZ))
    return jnp.cos(angle_value), -jnp.sin(angle_value)


def structure_factor(site_block, miller):
    return phase_angle(site_block, miller[0], miller[1], miller[2])


def projector_rows(site_block, kinds_block, beta_table, wave_miller):
    struct_re, struct_im = structure_factor(site_block, wave_miller)
    kind_onehot = (kinds_block[:, None] == jnp.arange(SPECIES, dtype=jnp.int32)[None, :]).astype(jnp.float32)
    table_three = beta_table.reshape(SPECIES, NH, -1)
    radial = jnp.einsum("as,sig->aig", kind_onehot, table_three, precision=highest)
    coef_real, coef_imag = phase_coefficients()
    part_re = radial * struct_re[:, None, :]
    part_im = radial * struct_im[:, None, :]
    vkb_re = coef_real[None, :, None] * part_re - coef_imag[None, :, None] * part_im
    vkb_im = coef_real[None, :, None] * part_im + coef_imag[None, :, None] * part_re
    return vkb_re.astype(jnp.bfloat16), vkb_im.astype(jnp.bfloat16)


def augment_weights(becsum, atom_kinds):
    pair_index, factors, parity = pair_tables(NH)
    kind_onehot = (atom_kinds[None, :] == jnp.arange(SPECIES, dtype=jnp.int32)[:, None]).astype(jnp.float32)
    parity_col = jnp.asarray(parity, jnp.float32)[:, None]
    even_rows = becsum.T * (1.0 - parity_col)
    odd_rows = -(becsum.T * parity_col)
    real_part = kind_onehot[:, None, :] * even_rows[None, :, :]
    imag_part = kind_onehot[:, None, :] * odd_rows[None, :, :]
    stacked = jnp.concatenate([real_part, imag_part], axis=2)
    return stacked.reshape(-1, stacked.shape[2]).astype(jnp.bfloat16)


def dense_augmentation(coefficients, atom_sites, column_x, column_y):
    slot_total = column_x.shape[0]
    zeros_z = jnp.zeros((1, NZ), jnp.int32)
    flat_x = (column_x[:, None] + zeros_z).reshape(-1).astype(jnp.int32)
    flat_y = (column_y[:, None] + zeros_z).reshape(-1).astype(jnp.int32)
    flat_z = (jnp.zeros((slot_total, 1), jnp.int32) + jnp.arange(NZ, dtype=jnp.int32)[None, :]).reshape(-1)
    struct_re, struct_im = phase_angle(atom_sites, flat_x, flat_y, flat_z)
    atom_total = coefficients.shape[0] // 2
    amp_re = coefficients[:atom_total]
    amp_im = coefficients[atom_total:]
    aug_re = jnp.sum(amp_re * struct_re - amp_im * struct_im, axis=0)
    aug_im = jnp.sum(amp_re * struct_im + amp_im * struct_re, axis=0)
    return aug_re.reshape(slot_total, NZ), aug_im.reshape(slot_total, NZ)


def reference(waves, occupations, beta_table, wave_miller, atom_kinds, atom_sites, aug_table, stick_columns):
    block_atoms = math.gcd(ATOMS, 8)
    wave_re = waves[0].astype(jnp.float32).T
    wave_im = waves[1].astype(jnp.float32).T

    def project_block(block_index):
        first_atom = block_index * block_atoms
        site_block = lax.dynamic_slice_in_dim(atom_sites, first_atom, block_atoms, 1)
        kinds_block = lax.dynamic_slice_in_dim(atom_kinds, first_atom, block_atoms, 0)
        vkb_re, vkb_im = projector_rows(site_block, kinds_block, beta_table, wave_miller)
        vkb_re = vkb_re.reshape(block_atoms * NH, -1).astype(jnp.float32)
        vkb_im = vkb_im.reshape(block_atoms * NH, -1).astype(jnp.float32)
        proj_re = jnp.dot(vkb_re, wave_re, precision=highest, preferred_element_type=jnp.float32) + jnp.dot(vkb_im, wave_im, precision=highest, preferred_element_type=jnp.float32)
        proj_im = jnp.dot(vkb_re, wave_im, precision=highest, preferred_element_type=jnp.float32) - jnp.dot(vkb_im, wave_re, precision=highest, preferred_element_type=jnp.float32)
        return proj_re.reshape(block_atoms, NH, -1), proj_im.reshape(block_atoms, NH, -1)

    becp_re, becp_im = lax.map(project_block, jnp.arange(ATOMS // block_atoms, dtype=jnp.int32))
    becp_re = becp_re.reshape(ATOMS, NH, -1)
    becp_im = becp_im.reshape(ATOMS, NH, -1)
    full_square = jnp.einsum("aic,ajc->aij", becp_re * occupations[None, None, :], becp_re, precision=highest)
    full_square = full_square + jnp.einsum("aic,ajc->aij", becp_im * occupations[None, None, :], becp_im, precision=highest)
    pair_index, factors, parity = pair_tables(NH)
    becsum = full_square.reshape(ATOMS, NH * NH)[:, pair_index] * factors[None, :]

    aug_weights = augment_weights(becsum, atom_kinds).astype(jnp.float32)
    stick_block = math.gcd(STICKS, 16)

    def dense_block(block_index):
        first_stick = block_index * stick_block
        columns = lax.dynamic_slice_in_dim(stick_columns, first_stick, stick_block, 0)
        table_block = lax.dynamic_slice_in_dim(aug_table, first_stick * NZ, stick_block * NZ, 1).astype(jnp.float32)
        stick_ids = first_stick + jnp.arange(stick_block, dtype=jnp.int32)
        column_x = (stick_ids // BLOCK_STICKS) * NXB + columns // NY
        column_y = columns % NY
        coefficients = jnp.dot(aug_weights.T, table_block, precision=highest, preferred_element_type=jnp.float32)
        aug_re, aug_im = dense_augmentation(coefficients, atom_sites, column_x, column_y)
        flat_rows = jnp.where(columns < 0, NX * NY, column_x * NY + column_y).astype(jnp.int32)
        return aug_re, aug_im, flat_rows

    aug_re, aug_im, flat_rows = lax.map(dense_block, jnp.arange(STICKS // stick_block, dtype=jnp.int32))
    flat_rows = flat_rows.reshape(-1)
    grid_re = jnp.zeros((NX * NY, NZ), jnp.float32).at[flat_rows].add(aug_re.reshape(-1, NZ), mode="drop")
    grid_im = jnp.zeros((NX * NY, NZ), jnp.float32).at[flat_rows].add(aug_im.reshape(-1, NZ), mode="drop")
    grid_values = lax.complex(grid_re, grid_im).reshape(NX, NY, NZ)
    density_field = jnp.fft.ifftn(grid_values) * (NX * NY * NZ)
    density_field = jnp.transpose(density_field, (2, 1, 0))
    return jnp.stack([jnp.real(density_field), jnp.imag(density_field)]).astype(jnp.float32)
```

```python
import functools
import math

import jax
import jax.numpy as jnp
import numpy as np
from jax import lax
from jax.experimental import pallas as pl
from jax.experimental.pallas import tpu as pltpu
from jax.sharding import PartitionSpec as P

NX = 240
NY = 240
NZ = 224
NH = 18
HALF = NH // 2
SPECIES = 4

PERIOD = math.lcm(NX, NY, NZ)
STEP_X = PERIOD // NX
STEP_Y = PERIOD // NY
STEP_Z = PERIOD // NZ
ELL = np.array([0, 0] + [1] * 6 + [2] * 10)
PAIR_FIRST, PAIR_SECOND = np.triu_indices(NH)

highest = lax.Precision.HIGHEST
F32 = jnp.float32
BF16 = jnp.bfloat16


def fit_even(func, terms):
    nodes = 0.125 * (1.0 + np.cos(np.pi * (np.arange(64) + 0.5) / 64))
    scaled = np.polynomial.chebyshev.Chebyshev.fit(nodes, func(np.sqrt(nodes)), terms - 1, domain=[0, 0.25])
    return [float(c) for c in scaled.convert(kind=np.polynomial.Polynomial).coef]


COS_FIT = fit_even(lambda u: np.cos(2 * np.pi * u), 7)
SIN_FIT = fit_even(lambda u: np.sin(2 * np.pi * u) / u, 6)


def horner(coefs, w):
    total = jnp.full_like(w, coefs[-1])
    for c in coefs[-2::-1]:
        total = total * w + c
    return total


def turn_cos_sin(count, period):
    rest = count - jnp.round(count * (1.0 / period)) * period
    u = rest * (1.0 / period)
    w = u * u
    return horner(COS_FIT, w), u * horner(SIN_FIT, w)


def projection_kernel(sites_ref, kinds_ref, miller_ref, beta_ref, wave_ref, out_ref, rows_ref):
    block = sites_ref.shape[0]
    width = miller_ref.shape[1]
    site = sites_ref[...]
    miller = miller_ref[...]
    count = site[:, 0:1] * miller[0:1, :] + site[:, 1:2] * miller[1:2, :] + site[:, 2:3] * miller[2:3, :]
    cosine, sine = turn_cos_sin(count, PERIOD)
    kinds = kinds_ref[...]
    masks = [kinds == s for s in range(1, SPECIES)]
    for i in range(NH):
        radial = jnp.broadcast_to(beta_ref[i : i + 1, :], (block, width))
        for s in range(1, SPECIES):
            radial = jnp.where(masks[s - 1], beta_ref[s * NH + i : s * NH + i + 1, :], radial)
        if ELL[i] == 0:
            real, imag = radial * cosine, -(radial * sine)
        elif ELL[i] == 1:
            real, imag = -(radial * sine), -(radial * cosine)
        else:
            real, imag = -(radial * cosine), radial * sine
        row = (i % HALF) * block
        col = (i // HALF) * 2 * width
        rows_ref[row : row + block, col : col + width] = real.astype(BF16)
        rows_ref[row : row + block, col + width : col + 2 * width] = imag.astype(BF16)
    result = jnp.dot(rows_ref[...], wave_ref[...], preferred_element_type=F32)
    out_ref[...] = result.reshape(HALF, block, result.shape[1])


def project(sites, kinds, miller, beta_table, wave_matrix):
    atoms = sites.shape[0]
    width = miller.shape[1]
    cols = wave_matrix.shape[1]
    block = math.gcd(atoms, 32)
    whole = lambda a: pl.BlockSpec(a.shape, lambda b: (0, 0))
    return pl.pallas_call(
        projection_kernel,
        grid=(atoms // block,),
        in_specs=[
            pl.BlockSpec((block, 3), lambda b: (b, 0)),
            pl.BlockSpec((block, 1), lambda b: (b, 0)),
            whole(miller),
            whole(beta_table),
            whole(wave_matrix),
        ],
        out_specs=pl.BlockSpec((HALF, block, cols), lambda b: (0, b, 0)),
        out_shape=jax.ShapeDtypeStruct((HALF, atoms, cols), F32),
        scratch_shapes=[pltpu.VMEM((HALF * block, 4 * width), BF16)],
        name="project",
    )(sites, kinds, miller, beta_table, wave_matrix)


def dense_kernel(weights_ref, table_ref, sites_ref, points_ref, out_ref):
    atoms = sites_ref.shape[0]
    coef = jnp.dot(weights_ref[...], table_ref[...], preferred_element_type=F32)
    site = sites_ref[...]
    points = points_ref[...]
    count = site[:, 0:1] * points[0:1, :] + site[:, 1:2] * points[1:2, :] + site[:, 2:3] * points[2:3, :]
    cosine, sine = turn_cos_sin(count, PERIOD)
    real, imag = coef[:atoms], coef[atoms:]
    out_ref[0:1, :] = jnp.sum(real * cosine + imag * sine, axis=0, keepdims=True)
    out_ref[1:2, :] = jnp.sum(imag * cosine - real * sine, axis=0, keepdims=True)


def dense(weights, table, sites, points):
    rows, cols = table.shape
    tile = math.gcd(cols, 256)
    return pl.pallas_call(
        dense_kernel,
        grid=(cols // tile,),
        in_specs=[
            pl.BlockSpec(weights.shape, lambda c: (0, 0)),
            pl.BlockSpec((rows, tile), lambda c: (0, c)),
            pl.BlockSpec(sites.shape, lambda c: (0, 0)),
            pl.BlockSpec((3, tile), lambda c: (0, c)),
        ],
        out_specs=pl.BlockSpec((2, tile), lambda c: (0, c)),
        out_shape=jax.ShapeDtypeStruct((2, cols), F32),
        name="dense",
    )(weights, table, sites, points)


def augment_weights(becsum, atom_kinds):
    odd = jnp.asarray((ELL[PAIR_FIRST] + ELL[PAIR_SECOND]) % 2 == 1)[None, :]
    even_rows = jnp.where(odd, 0.0, becsum)
    odd_rows = jnp.where(odd, -becsum, 0.0)
    stacked = jnp.concatenate([even_rows, odd_rows], axis=0).astype(BF16)
    kinds = jnp.concatenate([atom_kinds, atom_kinds])[:, None]
    parts = [jnp.where(kinds == s, stacked, jnp.zeros_like(stacked)) for s in range(SPECIES)]
    return jnp.concatenate(parts, axis=1)


def table_of(rows, cols, period):
    angle = (np.outer(rows, cols) % period) * (2.0 * np.pi / period)
    return np.cos(angle).astype(np.float32), np.sin(angle).astype(np.float32)


def on_device(
    waves, occupations, beta_table, wave_miller, atom_kinds, atom_sites, aug_table, stick_columns
):
    bands = lax.axis_size("band")
    groups = lax.axis_size("ga")
    atoms = atom_sites.shape[1]
    slots = stick_columns.shape[0]
    column_block = NX // bands
    y_block = NY // bands
    planes = NZ // groups
    steps = jnp.asarray([STEP_X, STEP_Y, STEP_Z], F32)
    sites = atom_sites.T.astype(F32) * steps[None, :]

    wave_t = jnp.concatenate(
        [
            jnp.concatenate([waves[0], waves[1]], axis=1),
            jnp.concatenate([waves[1], -waves[0]], axis=1),
        ],
        axis=0,
    ).T
    empty = jnp.zeros_like(wave_t)
    wave_matrix = jnp.concatenate(
        [jnp.concatenate([wave_t, empty], axis=1), jnp.concatenate([empty, wave_t], axis=1)], axis=0
    )
    pieces = project(sites, atom_kinds[:, None], wave_miller.astype(F32), beta_table, wave_matrix)
    own = lax.psum_scatter(pieces, "ga", scatter_dimension=1, tiled=True)
    own_atoms = own.shape[1]
    blocks = own.reshape(HALF, own_atoms, 2, wave_t.shape[1]).transpose(1, 2, 0, 3)
    blocks = blocks.reshape(own_atoms, NH, wave_t.shape[1])
    occupied = jnp.concatenate([occupations, occupations])
    square = jnp.einsum("aic,ajc->aij", blocks * occupied[None, None, :], blocks, precision=highest)
    factors = np.where(PAIR_FIRST == PAIR_SECOND, 1.0, 2.0).astype(np.float32)
    partial_value = square.reshape(own_atoms, NH * NH)[:, PAIR_FIRST * NH + PAIR_SECOND] * factors[None, :]
    becsum = lax.all_gather(lax.psum(partial_value, "band"), "ga", axis=0, tiled=True)
    weights = augment_weights(becsum, atom_kinds)

    column_x = lax.axis_index("band") * column_block + stick_columns // NY
    column_y = stick_columns % NY
    ones_z = jnp.ones((1, NZ), jnp.int32)
    points = jnp.stack(
        [
            (column_x[:, None] * ones_z).reshape(-1),
            (column_y[:, None] * ones_z).reshape(-1),
            (jnp.arange(NZ, dtype=jnp.int32)[None, :] + jnp.zeros((slots, 1), jnp.int32)).reshape(-1),
        ]
    ).astype(F32)
    aug = dense(weights, aug_table, sites, points).reshape(2, slots, NZ)
    cos_z, sin_z = table_of(np.arange(NZ), np.arange(NZ), NZ)
    both = jnp.dot(aug.reshape(2 * slots, NZ), np.concatenate([cos_z, sin_z], axis=1), precision=highest)
    both = both.reshape(2, slots, 2, NZ)
    stick_re = both[0, :, 0] - both[1, :, 1]
    stick_im = both[0, :, 1] + both[1, :, 0]
    packed = jnp.concatenate(
        [
            stick_re.reshape(slots, groups, planes),
            stick_im.reshape(slots, groups, planes),
            jnp.broadcast_to(stick_columns.astype(F32)[:, None, None], (slots, groups, 1)),
        ],
        axis=2,
    ).transpose(1, 0, 2)
    received = lax.all_to_all(packed, "ga", split_axis=0, concat_axis=0, tiled=True)
    received = lax.all_gather(received.reshape(groups * slots, -1), "band", axis=0, tiled=True)
    return finish(received, planes, y_block, column_block, groups * slots)


def finish(received, planes, y_block, column_block, block_sticks):
    total = received.shape[0]
    columns = received[:, 2 * planes]
    live = columns >= 0
    value_re = jnp.where(live[:, None], received[:, :planes], 0.0)
    value_im = jnp.where(live[:, None], received[:, planes : 2 * planes], 0.0)
    columns = columns.astype(jnp.int32)
    gx = ((jnp.arange(total, dtype=jnp.int32) // block_sticks) * column_block + columns // NY).astype(F32)
    gy = (columns % NY).astype(F32)
    y_values = (lax.axis_index("band") * y_block + jnp.arange(y_block, dtype=jnp.int32)).astype(F32)
    cos_y, sin_y = turn_cos_sin(gy[:, None] * y_values[None, :], NY)
    cos_x, sin_x = turn_cos_sin(gx[:, None] * jnp.arange(NX, dtype=jnp.int32).astype(F32)[None, :], NX)
    amp_re = value_re[:, :, None] * cos_y[:, None, :] - value_im[:, :, None] * sin_y[:, None, :]
    amp_im = value_re[:, :, None] * sin_y[:, None, :] + value_im[:, :, None] * cos_y[:, None, :]
    amp = jnp.concatenate([amp_re, amp_im], axis=0)
    dims = (((0,), (0,)), ((), ()))
    wave_re = jnp.concatenate([cos_x, -sin_x], axis=0)
    wave_im = jnp.concatenate([sin_x, cos_x], axis=0)
    out_re = lax.dot_general(amp, wave_re, dims, precision=lax.Precision.HIGH)
    out_im = lax.dot_general(amp, wave_im, dims, precision=lax.Precision.HIGH)
    return jnp.stack([out_re, out_im])


def solution(mesh):
    in_specs = (
        P(None, "band", "ga"),
        P("band"),
        P(None, "ga"),
        P(None, "ga"),
        P(),
        P(),
        P(None, ("band", "ga")),
        P(("band", "ga")),
    )
    out_specs = P(None, "ga", "band", None)
    return jax.shard_map(
        on_device, mesh=mesh, in_specs=in_specs, out_specs=out_specs, check_vma=False
    )
```

```python
import functools
import math

import jax
import jax.numpy as jnp
import numpy as np
from jax import lax
from jax.experimental import pallas as pl
from jax.experimental.pallas import tpu as pltpu
from jax.sharding import PartitionSpec as P

NX = 240
NY = 240
NZ = 224
NH = 18
HALF = NH // 2
SPECIES = 4

PERIOD = math.lcm(NX, NY, NZ)
STEP_X = PERIOD // NX
STEP_Y = PERIOD // NY
STEP_Z = PERIOD // NZ
ELL = np.array([0, 0] + [1] * 6 + [2] * 10)
PAIR_FIRST, PAIR_SECOND = np.triu_indices(NH)

highest = lax.Precision.HIGHEST
F32 = jnp.float32
BF16 = jnp.bfloat16


def fit_even(func, terms):
    nodes = 0.125 * (1.0 + np.cos(np.pi * (np.arange(64) + 0.5) / 64))
    scaled = np.polynomial.chebyshev.Chebyshev.fit(nodes, func(np.sqrt(nodes)), terms - 1, domain=[0, 0.25])
    return [float(c) for c in scaled.convert(kind=np.polynomial.Polynomial).coef]


COS_FIT = fit_even(lambda u: np.cos(2 * np.pi * u), 7)
SIN_FIT = fit_even(lambda u: np.sin(2 * np.pi * u) / u, 6)


def horner(coefs, w):
    total = jnp.full_like(w, coefs[-1])
    for c in coefs[-2::-1]:
        total = total * w + c
    return total


def turn_cos_sin(count, period):
    rest = count - jnp.round(count * (1.0 / period)) * period
    u = rest * (1.0 / period)
    w = u * u
    return horner(COS_FIT, w), u * horner(SIN_FIT, w)


MESH = pl.DeviceIdType.MESH


def greet(peers, axis_sets):
    barrier = pltpu.get_barrier_semaphore()
    for count, device_of in axis_sets:

        @pl.loop(1, count)
        def _(step):
            pl.semaphore_signal(barrier, inc=1, device_id=device_of(step), device_id_type=MESH)

    pl.semaphore_wait(barrier, peers)


def group_peer(groups):
    band, me = lax.axis_index("band"), lax.axis_index("ga")
    return lambda step: (band, lax.rem(me + step, groups))


def band_peer(bands):
    band, me = lax.axis_index("band"), lax.axis_index("ga")
    return lambda step: (lax.rem(band + step, bands), me)


def projection_kernel(
    groups,
    own,
    sites_ref,
    kinds_ref,
    miller_ref,
    beta_ref,
    wave_ref,
    out_ref,
    rows_ref,
    send_ref,
    recv_ref,
    send_sem,
    recv_sem,
):
    band, me = lax.axis_index("band"), lax.axis_index("ga")
    width = miller_ref.shape[1]
    steps, _, block, cols = send_ref.shape
    ratio = block // own
    greet(groups - 1, [(groups, group_peer(groups))])

    def copy_to(index, part, target):
        return pltpu.make_async_remote_copy(
            src_ref=send_ref.at[index, :, pl.ds(pl.multiple_of(part * own, own), own), :],
            dst_ref=recv_ref.at[me],
            send_sem=send_sem.at[target],
            recv_sem=recv_sem.at[me],
            device_id=(band, target),
            device_id_type=MESH,
        )

    @pl.loop(0, steps)
    def _(step):
        index = lax.rem(me // ratio + 1 + step, steps)
        start = pl.multiple_of(index * block, block)
        site = sites_ref[pl.ds(start, block), :]
        kinds = kinds_ref[pl.ds(start, block), :]
        miller = miller_ref[...]
        count = site[:, 0:1] * miller[0:1, :] + site[:, 1:2] * miller[1:2, :] + site[:, 2:3] * miller[2:3, :]
        cosine, sine = turn_cos_sin(count, PERIOD)
        masks = [kinds == s for s in range(1, SPECIES)]
        for i in range(NH):
            radial = jnp.broadcast_to(beta_ref[i : i + 1, :], (block, width))
            for s in range(1, SPECIES):
                radial = jnp.where(masks[s - 1], beta_ref[s * NH + i : s * NH + i + 1, :], radial)
            if ELL[i] == 0:
                real, imag = radial * cosine, -(radial * sine)
            elif ELL[i] == 1:
                real, imag = -(radial * sine), -(radial * cosine)
            else:
                real, imag = -(radial * cosine), radial * sine
            row = (i % HALF) * block
            col = (i // HALF) * 2 * width
            rows_ref[row : row + block, col : col + width] = real.astype(BF16)
            rows_ref[row : row + block, col + width : col + 2 * width] = imag.astype(BF16)
        result = jnp.dot(rows_ref[...], wave_ref[...], preferred_element_type=F32)
        send_ref[index] = result.reshape(HALF, block, cols)
        for part in range(ratio):
            target = index * ratio + part

            @pl.when(target != me)
            def _():
                copy_to(index, part, target).start()

    total = send_ref[me // ratio, :, pl.ds(pl.multiple_of(lax.rem(me, ratio) * own, own), own), :]
    for step in range(1, groups):
        source = lax.rem(me + step, groups)
        pltpu.make_async_remote_copy(
            src_ref=send_ref.at[0, :, pl.ds(0, own), :],
            dst_ref=recv_ref.at[source],
            send_sem=send_sem.at[source],
            recv_sem=recv_sem.at[source],
            device_id=(band, source),
            device_id_type=MESH,
        ).wait_recv()
        total = total + recv_ref[source]
    out_ref[...] = total

    @pl.loop(1, groups)
    def _(step):
        target = lax.rem(me + step, groups)
        copy_to(0, 0, target).wait_send()


def project(sites, kinds, miller, beta_table, wave_matrix, groups):
    atoms = sites.shape[0]
    width = miller.shape[1]
    cols = wave_matrix.shape[1]
    own = atoms // groups
    block = own * max(1, 32 // own)
    steps = atoms // block
    return pl.pallas_call(
        functools.partial(projection_kernel, groups, own),
        in_specs=[pl.BlockSpec(memory_space=pltpu.VMEM)] * 5,
        out_specs=pl.BlockSpec(memory_space=pltpu.VMEM),
        out_shape=jax.ShapeDtypeStruct((HALF, own, cols), F32),
        scratch_shapes=[
            pltpu.VMEM((HALF * block, 4 * width), BF16),
            pltpu.VMEM((steps, HALF, block, cols), F32),
            pltpu.VMEM((groups, HALF, own, cols), F32),
            pltpu.SemaphoreType.DMA((groups,)),
            pltpu.SemaphoreType.DMA((groups,)),
        ],
        compiler_params=pltpu.CompilerParams(collective_id=0, has_side_effects=True),
        name="project",
    )(sites, kinds, miller, beta_table, wave_matrix)


def becsum_kernel(bands, groups, part_ref, out_ref, recv_ref, sum_ref, band_send, band_recv, send_sem, recv_sem):
    band, me = lax.axis_index("band"), lax.axis_index("ga")
    to_band, to_group = band_peer(bands), group_peer(groups)
    greet(bands + groups - 2, [(bands, to_band), (groups, to_group)])

    def band_copy(step, slot):
        return pltpu.make_async_remote_copy(
            src_ref=part_ref,
            dst_ref=recv_ref.at[slot],
            send_sem=band_send.at[step],
            recv_sem=band_recv.at[slot],
            device_id=to_band(step),
            device_id_type=MESH,
        )

    def group_copy(step, slot):
        return pltpu.make_async_remote_copy(
            src_ref=sum_ref,
            dst_ref=out_ref.at[slot],
            send_sem=send_sem.at[step],
            recv_sem=recv_sem.at[slot],
            device_id=to_group(step),
            device_id_type=MESH,
        )

    for step in range(1, bands):
        band_copy(step, band).start()
    recv_ref[band] = part_ref[...]
    for step in range(1, bands):
        band_copy(step, lax.rem(band + step, bands)).wait_recv()
    total = recv_ref[0]
    for source in range(1, bands):
        total = total + recv_ref[source]
    sum_ref[...] = total
    for step in range(1, groups):
        group_copy(step, me).start()
    out_ref[me] = total
    for step in range(1, bands):
        band_copy(step, band).wait_send()
    for step in range(1, groups):
        group_copy(step, lax.rem(me + step, groups)).wait_recv()
    for step in range(1, groups):
        group_copy(step, me).wait_send()


def gather_becsum(part, bands, groups):
    return pl.pallas_call(
        functools.partial(becsum_kernel, bands, groups),
        in_specs=[pl.BlockSpec(memory_space=pltpu.VMEM)],
        out_specs=pl.BlockSpec(memory_space=pltpu.VMEM),
        out_shape=jax.ShapeDtypeStruct((groups,) + part.shape, F32),
        scratch_shapes=[
            pltpu.VMEM((bands,) + part.shape, F32),
            pltpu.VMEM(part.shape, F32),
            pltpu.SemaphoreType.DMA((bands,)),
            pltpu.SemaphoreType.DMA((bands,)),
            pltpu.SemaphoreType.DMA((groups,)),
            pltpu.SemaphoreType.DMA((groups,)),
        ],
        compiler_params=pltpu.CompilerParams(collective_id=1, has_side_effects=True),
        name="gather_becsum",
    )(part)


def sticks_kernel(bands, groups, part_ref, out_ref, send_sem, recv_sem):
    band, me = lax.axis_index("band"), lax.axis_index("ga")
    place = band * groups + me
    devices = bands * groups

    def peer(step):
        other = lax.rem(place + step, devices)
        return other // groups, lax.rem(other, groups)

    greet(devices - 1, [(devices, peer)])

    def copy(step, slot):
        target = peer(step)
        return pltpu.make_async_remote_copy(
            src_ref=part_ref.at[target[1]],
            dst_ref=out_ref.at[slot],
            send_sem=send_sem.at[step],
            recv_sem=recv_sem.at[slot],
            device_id=target,
            device_id_type=MESH,
        )

    @pl.loop(1, devices)
    def _(step):
        copy(step, place).start()

    out_ref[place] = part_ref[me]

    @pl.loop(1, devices)
    def _(step):
        copy(step, lax.rem(place + step, devices)).wait_recv()

    @pl.loop(1, devices)
    def _(step):
        copy(step, place).wait_send()


def exchange_sticks(part, bands, groups):
    devices = bands * groups
    return pl.pallas_call(
        functools.partial(sticks_kernel, bands, groups),
        in_specs=[pl.BlockSpec(memory_space=pltpu.VMEM)],
        out_specs=pl.BlockSpec(memory_space=pltpu.VMEM),
        out_shape=jax.ShapeDtypeStruct((devices,) + part.shape[1:], F32),
        scratch_shapes=[
            pltpu.SemaphoreType.DMA((devices,)),
            pltpu.SemaphoreType.DMA((devices,)),
        ],
        compiler_params=pltpu.CompilerParams(collective_id=2, has_side_effects=True),
        name="exchange_sticks",
    )(part)


def dense_kernel(weights_ref, table_ref, sites_ref, points_ref, out_ref):
    atoms = sites_ref.shape[0]
    coef = jnp.dot(weights_ref[...], table_ref[...], preferred_element_type=F32)
    site = sites_ref[...]
    points = points_ref[...]
    count = site[:, 0:1] * points[0:1, :] + site[:, 1:2] * points[1:2, :] + site[:, 2:3] * points[2:3, :]
    cosine, sine = turn_cos_sin(count, PERIOD)
    real, imag = coef[:atoms], coef[atoms:]
    out_ref[0:1, :] = jnp.sum(real * cosine + imag * sine, axis=0, keepdims=True)
    out_ref[1:2, :] = jnp.sum(imag * cosine - real * sine, axis=0, keepdims=True)


def dense(weights, table, sites, points):
    rows, cols = table.shape
    tile = math.gcd(cols, 256)
    return pl.pallas_call(
        dense_kernel,
        grid=(cols // tile,),
        in_specs=[
            pl.BlockSpec(weights.shape, lambda c: (0, 0)),
            pl.BlockSpec((rows, tile), lambda c: (0, c)),
            pl.BlockSpec(sites.shape, lambda c: (0, 0)),
            pl.BlockSpec((3, tile), lambda c: (0, c)),
        ],
        out_specs=pl.BlockSpec((2, tile), lambda c: (0, c)),
        out_shape=jax.ShapeDtypeStruct((2, cols), F32),
        name="dense",
    )(weights, table, sites, points)


def augment_weights(becsum, atom_kinds):
    odd = jnp.asarray((ELL[PAIR_FIRST] + ELL[PAIR_SECOND]) % 2 == 1)[None, :]
    even_rows = jnp.where(odd, 0.0, becsum)
    odd_rows = jnp.where(odd, -becsum, 0.0)
    stacked = jnp.concatenate([even_rows, odd_rows], axis=0).astype(BF16)
    kinds = jnp.concatenate([atom_kinds, atom_kinds])[:, None]
    parts = [jnp.where(kinds == s, stacked, jnp.zeros_like(stacked)) for s in range(SPECIES)]
    return jnp.concatenate(parts, axis=1)


def table_of(rows, cols, period):
    angle = (np.outer(rows, cols) % period) * (2.0 * np.pi / period)
    return np.cos(angle).astype(np.float32), np.sin(angle).astype(np.float32)


def on_device(
    waves, occupations, beta_table, wave_miller, atom_kinds, atom_sites, aug_table, stick_columns
):
    bands = lax.axis_size("band")
    groups = lax.axis_size("ga")
    atoms = atom_sites.shape[1]
    slots = stick_columns.shape[0]
    column_block = NX // bands
    y_block = NY // bands
    planes = NZ // groups
    steps = jnp.asarray([STEP_X, STEP_Y, STEP_Z], F32)
    sites = atom_sites.T.astype(F32) * steps[None, :]

    wave_t = jnp.concatenate(
        [
            jnp.concatenate([waves[0], waves[1]], axis=1),
            jnp.concatenate([waves[1], -waves[0]], axis=1),
        ],
        axis=0,
    ).T
    empty = jnp.zeros_like(wave_t)
    wave_matrix = jnp.concatenate(
        [jnp.concatenate([wave_t, empty], axis=1), jnp.concatenate([empty, wave_t], axis=1)], axis=0
    )
    own = project(sites, atom_kinds[:, None], wave_miller.astype(F32), beta_table, wave_matrix, groups)
    own_atoms = own.shape[1]
    blocks = own.reshape(HALF, own_atoms, 2, wave_t.shape[1]).transpose(1, 2, 0, 3)
    blocks = blocks.reshape(own_atoms, NH, wave_t.shape[1])
    occupied = jnp.concatenate([occupations, occupations])
    square = jnp.einsum("aic,ajc->aij", blocks * occupied[None, None, :], blocks, precision=highest)
    factors = np.where(PAIR_FIRST == PAIR_SECOND, 1.0, 2.0).astype(np.float32)
    partial_value = square.reshape(own_atoms, NH * NH)[:, PAIR_FIRST * NH + PAIR_SECOND] * factors[None, :]
    becsum = gather_becsum(partial_value, bands, groups).reshape(atoms, -1)
    weights = augment_weights(becsum, atom_kinds)

    column_x = lax.axis_index("band") * column_block + stick_columns // NY
    column_y = stick_columns % NY
    ones_z = jnp.ones((1, NZ), jnp.int32)
    points = jnp.stack(
        [
            (column_x[:, None] * ones_z).reshape(-1),
            (column_y[:, None] * ones_z).reshape(-1),
            (jnp.arange(NZ, dtype=jnp.int32)[None, :] + jnp.zeros((slots, 1), jnp.int32)).reshape(-1),
        ]
    ).astype(F32)
    aug = dense(weights, aug_table, sites, points).reshape(2, slots, NZ)
    lines = aug.transpose(1, 0, 2).reshape(slots, 2 * NZ)
    cos_z, sin_z = table_of(np.arange(NZ), np.arange(NZ), NZ)
    lanes = 128 * (-(-(2 * planes + 1) // 128))
    spread = np.zeros((2, NZ, groups, lanes), np.float32)
    spread[0, :, :, :planes] = cos_z.reshape(NZ, groups, planes)
    spread[1, :, :, :planes] = -sin_z.reshape(NZ, groups, planes)
    spread[0, :, :, planes : 2 * planes] = sin_z.reshape(NZ, groups, planes)
    spread[1, :, :, planes : 2 * planes] = cos_z.reshape(NZ, groups, planes)
    packed = jnp.dot(lines, spread.reshape(2 * NZ, groups * lanes), precision=highest)
    packed = packed.reshape(slots, groups, lanes).transpose(1, 0, 2)
    at_column = jnp.arange(lanes)[None, None, :] == 2 * planes
    packed = jnp.where(at_column, stick_columns.astype(F32)[None, :, None], packed)
    received = exchange_sticks(packed, bands, groups).reshape(bands * groups * slots, lanes)
    return finish(received, planes, y_block, column_block, groups * slots)


def finish(received, planes, y_block, column_block, block_sticks):
    total = received.shape[0]
    columns = received[:, 2 * planes]
    live = columns >= 0
    value_re = jnp.where(live[:, None], received[:, :planes], 0.0)
    value_im = jnp.where(live[:, None], received[:, planes : 2 * planes], 0.0)
    columns = columns.astype(jnp.int32)
    gx = ((jnp.arange(total, dtype=jnp.int32) // block_sticks) * column_block + columns // NY).astype(F32)
    gy = (columns % NY).astype(F32)
    y_values = (lax.axis_index("band") * y_block + jnp.arange(y_block, dtype=jnp.int32)).astype(F32)
    cos_y, sin_y = turn_cos_sin(gy[:, None] * y_values[None, :], NY)
    cos_x, sin_x = turn_cos_sin(gx[:, None] * jnp.arange(NX, dtype=jnp.int32).astype(F32)[None, :], NX)
    amp_re = value_re[:, :, None] * cos_y[:, None, :] - value_im[:, :, None] * sin_y[:, None, :]
    amp_im = value_re[:, :, None] * sin_y[:, None, :] + value_im[:, :, None] * cos_y[:, None, :]
    amp = jnp.concatenate([amp_re, amp_im], axis=0)
    dims = (((0,), (0,)), ((), ()))
    wave_re = jnp.concatenate([cos_x, -sin_x], axis=0)
    wave_im = jnp.concatenate([sin_x, cos_x], axis=0)
    out_re = lax.dot_general(amp, wave_re, dims, precision=lax.Precision.HIGH)
    out_im = lax.dot_general(amp, wave_im, dims, precision=lax.Precision.HIGH)
    return jnp.stack([out_re, out_im])


def solution(mesh):
    in_specs = (
        P(None, "band", "ga"),
        P("band"),
        P(None, "ga"),
        P(None, "ga"),
        P(),
        P(),
        P(None, ("band", "ga")),
        P(("band", "ga")),
    )
    out_specs = P(None, "ga", "band", None)
    return jax.shard_map(
        on_device, mesh=mesh, in_specs=in_specs, out_specs=out_specs, check_vma=False
    )
```

```python
import functools
import math

import jax
import jax.numpy as jnp
import numpy as np
from jax import lax
from jax.experimental import pallas as pl
from jax.experimental.pallas import tpu as pltpu
from jax.sharding import PartitionSpec as P

NX = 240
NY = 240
NZ = 224
NH = 18
HALF = NH // 2
SPECIES = 4

PERIOD = math.lcm(NX, NY, NZ)
STEP_X = PERIOD // NX
STEP_Y = PERIOD // NY
STEP_Z = PERIOD // NZ
ELL = np.array([0, 0] + [1] * 6 + [2] * 10)
PAIR_FIRST, PAIR_SECOND = np.triu_indices(NH)

highest = lax.Precision.HIGHEST
F32 = jnp.float32
BF16 = jnp.bfloat16


def fit_even(func, terms):
    nodes = 0.125 * (1.0 + np.cos(np.pi * (np.arange(64) + 0.5) / 64))
    scaled = np.polynomial.chebyshev.Chebyshev.fit(nodes, func(np.sqrt(nodes)), terms - 1, domain=[0, 0.25])
    return [float(c) for c in scaled.convert(kind=np.polynomial.Polynomial).coef]


COS_FIT = fit_even(lambda u: np.cos(2 * np.pi * u), 7)
SIN_FIT = fit_even(lambda u: np.sin(2 * np.pi * u) / u, 6)


def horner(coefs, w):
    total = jnp.full_like(w, coefs[-1])
    for c in coefs[-2::-1]:
        total = total * w + c
    return total


def turn_cos_sin(count, period):
    rest = count - jnp.round(count * (1.0 / period)) * period
    u = rest * (1.0 / period)
    w = u * u
    return horner(COS_FIT, w), u * horner(SIN_FIT, w)


MESH = pl.DeviceIdType.MESH


def greet(peers, axis_sets):
    barrier = pltpu.get_barrier_semaphore()
    for count, device_of in axis_sets:

        @pl.loop(1, count)
        def _(step):
            pl.semaphore_signal(barrier, inc=1, device_id=device_of(step), device_id_type=MESH)

    pl.semaphore_wait(barrier, peers)


def up(value, unit):
    return -(-value // unit) * unit


def split(value):
    high = value.astype(BF16)
    return high, (value - high.astype(F32)).astype(BF16)


def mega_kernel(
    bands,
    groups,
    waves_ref,
    occ_ref,
    beta_ref,
    miller_ref,
    kinds_ref,
    site_ref,
    columns_ref,
    signs_ref,
    table_hbm,
    spread_hbm,
    out_ref,
    small_ref,
    site_t_ref,
    wave_ref,
    rows_ref,
    send_ref,
    recv_ref,
    phase_ref,
    total_ref,
    part_ref,
    band_ref,
    pair_ref,
    pack_ref,
    all_ref,
    weights_ref,
    table_ref,
    spread_ref,
    aug_ref,
    lines_ref,
    stick_ref,
    rs_send,
    rs_recv,
    band_send,
    band_recv,
    ga_send,
    ga_recv,
    dev_send,
    dev_recv,
    local_sem,
):
    band, me = lax.axis_index("band"), lax.axis_index("ga")
    devices = bands * groups
    place = band * groups + me
    atoms = site_ref.shape[1]
    own = atoms // groups
    width = miller_ref.shape[1]
    nb = waves_ref.shape[1]
    slots = columns_ref.shape[0]
    steps, _, block, cols = send_ref.shape
    ratio = block // own
    points = slots * NZ
    tile = phase_ref.shape[-1]
    planes = NZ // groups
    lanes = stick_ref.shape[-1]
    pairs = len(PAIR_FIRST)

    table_copy = pltpu.make_async_copy(table_hbm, table_ref, local_sem.at[0])
    spread_copy = pltpu.make_async_copy(spread_hbm, spread_ref, local_sem.at[1])
    table_copy.start()
    spread_copy.start()

    def peer(step):
        other = lax.rem(place + step, devices)
        return other // groups, lax.rem(other, groups)

    greet(devices - 1, [(devices, peer)])

    small_ref[...] = jnp.zeros_like(small_ref)
    small_ref[0:1, :] = site_ref[0:1, :].astype(F32) * STEP_X
    small_ref[1:2, :] = site_ref[1:2, :].astype(F32) * STEP_Y
    small_ref[2:3, :] = site_ref[2:3, :].astype(F32) * STEP_Z
    small_ref[3:4, :] = kinds_ref[...].astype(F32)
    small_ref[4:5, 0:nb] = occ_ref[...]
    small_ref[4:5, nb : 2 * nb] = occ_ref[...]
    site_t_ref[...] = jnp.swapaxes(small_ref[...], 0, 1)

    wave_ref[...] = jnp.zeros_like(wave_ref)
    re, im = waves_ref[0], waves_ref[1]
    for h in range(2):
        r, c = 2 * nb * h, 2 * width * h
        wave_ref[r : r + nb, c : c + width] = re
        wave_ref[r : r + nb, c + width : c + 2 * width] = im
        wave_ref[r + nb : r + 2 * nb, c : c + width] = im
        wave_ref[r + nb : r + 2 * nb, c + width : c + 2 * width] = -re

    def rs_copy(index, part, target, slot):
        return pltpu.make_async_remote_copy(
            src_ref=send_ref.at[index, :, pl.ds(pl.multiple_of(part * own, own), own), :],
            dst_ref=recv_ref.at[slot],
            send_sem=rs_send.at[target],
            recv_sem=rs_recv.at[slot],
            device_id=(band, target),
            device_id_type=MESH,
        )

    @pl.loop(0, steps)
    def _(step):
        index = lax.rem(me // ratio + 1 + step, steps)
        start = pl.multiple_of(index * block, block)
        site = site_t_ref[pl.ds(start, block), :]
        kinds = site[:, 3:4]
        miller = miller_ref[...].astype(F32)
        count = site[:, 0:1] * miller[0:1, :] + site[:, 1:2] * miller[1:2, :] + site[:, 2:3] * miller[2:3, :]
        cosine, sine = turn_cos_sin(count, PERIOD)
        masks = [kinds == float(s) for s in range(1, SPECIES)]
        for i in range(NH):
            radial = jnp.broadcast_to(beta_ref[i : i + 1, :], (block, width))
            for s in range(1, SPECIES):
                radial = jnp.where(masks[s - 1], beta_ref[s * NH + i : s * NH + i + 1, :], radial)
            if ELL[i] == 0:
                real, imag = radial * cosine, -(radial * sine)
            elif ELL[i] == 1:
                real, imag = -(radial * sine), -(radial * cosine)
            else:
                real, imag = -(radial * cosine), radial * sine
            row = (i % HALF) * block
            col = (i // HALF) * 2 * width
            rows_ref[row : row + block, col : col + width] = real.astype(BF16)
            rows_ref[row : row + block, col + width : col + 2 * width] = imag.astype(BF16)
        result = lax.dot_general(
            rows_ref[...], wave_ref[...], (((1,), (1,)), ((), ())), preferred_element_type=F32
        )
        send_ref[index] = result.reshape(HALF, block, cols)
        for part in range(ratio):
            target = index * ratio + part

            @pl.when(target != me)
            def _():
                rs_copy(index, part, target, me).start()

    @pl.loop(0, points // tile)
    def _(step):
        point = step * tile + lax.broadcasted_iota(jnp.int32, (1, tile), 1)
        x_row = jnp.zeros((1, tile), F32)
        y_row = jnp.zeros((1, tile), F32)
        z_row = point.astype(F32)
        for t in range(slots):
            column = columns_ref[t]
            x = band * (NX // bands) + lax.div(column, NY)
            y = lax.rem(column, NY)
            inside = point >= t * NZ
            x_row = jnp.where(inside, x.astype(F32), x_row)
            y_row = jnp.where(inside, y.astype(F32), y_row)
            z_row = jnp.where(inside, (point - t * NZ).astype(F32), z_row)
        count = site_t_ref[:, 0:1] * x_row + site_t_ref[:, 1:2] * y_row + site_t_ref[:, 2:3] * z_row
        cosine, sine = turn_cos_sin(count, PERIOD)
        phase_ref[step, 0] = cosine
        phase_ref[step, 1] = sine

    total = send_ref[me // ratio, :, pl.ds(pl.multiple_of(lax.rem(me, ratio) * own, own), own), :]
    for step in range(1, groups):
        source = lax.rem(me + step, groups)
        rs_copy(0, 0, source, source).wait_recv()
        total = total + recv_ref[source]

    total_ref[...] = jnp.zeros_like(total_ref)
    total_ref[0 : HALF * own, :] = total.reshape(HALF * own, cols)
    turned = jnp.swapaxes(total_ref[...], 0, 1)
    becp = jnp.concatenate([turned[0 : 2 * nb, : HALF * own], turned[2 * nb :, : HALF * own]], axis=1)
    scaled = becp * site_t_ref[0 : 2 * nb, 4:5]
    part_ref[...] = jnp.zeros_like(part_ref)
    for d in range(NH):
        size = (NH - d) * own
        product = scaled[:, :size] * becp[:, d * own :]
        part_ref[d : d + 1, 0:size] = jnp.sum(product, axis=0, keepdims=True)

    def band_copy(step, slot):
        return pltpu.make_async_remote_copy(
            src_ref=part_ref,
            dst_ref=band_ref.at[slot],
            send_sem=band_send.at[step],
            recv_sem=band_recv.at[slot],
            device_id=(lax.rem(band + step, bands), me),
            device_id_type=MESH,
        )

    for step in range(1, bands):
        band_copy(step, band).start()
    band_ref[band] = part_ref[...]
    for step in range(1, bands):
        band_copy(step, lax.rem(band + step, bands)).wait_recv()
    summed = band_ref[0]
    for source in range(1, bands):
        summed = summed + band_ref[source]

    pair_ref[...] = jnp.zeros_like(pair_ref)
    begin = 0
    for i in range(NH):
        pair_ref[begin : begin + NH - i, :] = summed[: NH - i, i * own : (i + 1) * own]
        begin += NH - i
    chunk = pack_ref.shape[0]
    chunks = pack_ref.shape[1] // own
    pack_ref[...] = jnp.concatenate(
        [pair_ref[q * chunk : (q + 1) * chunk, :] for q in range(chunks)], axis=1
    )

    def ga_copy(step, slot):
        return pltpu.make_async_remote_copy(
            src_ref=pack_ref,
            dst_ref=all_ref.at[slot],
            send_sem=ga_send.at[step],
            recv_sem=ga_recv.at[slot],
            device_id=(band, lax.rem(me + step, groups)),
            device_id_type=MESH,
        )

    for step in range(1, groups):
        ga_copy(step, me).start()
    all_ref[me] = pack_ref[...]
    for step in range(1, groups):
        ga_copy(step, lax.rem(me + step, groups)).wait_recv()
    becsum = jnp.concatenate(
        [
            jnp.concatenate([all_ref[g, :, q * own : (q + 1) * own] for g in range(groups)], axis=1)
            for q in range(chunks)
        ],
        axis=0,
    )[:pairs]
    even = becsum * signs_ref[:, 0:1]
    odd = becsum * signs_ref[:, 1:2]
    kind_row = small_ref[3:4, :]
    weights_ref[...] = jnp.zeros_like(weights_ref)
    for s in range(SPECIES):
        here = kind_row == float(s)
        weights_ref[s * pairs : (s + 1) * pairs, 0:atoms] = jnp.where(here, even, 0.0)
        weights_ref[s * pairs : (s + 1) * pairs, atoms : 2 * atoms] = jnp.where(here, odd, 0.0)
    weights = jnp.swapaxes(weights_ref[...], 0, 1).astype(BF16)[:, : SPECIES * pairs]

    table_copy.wait()
    for step in range(points // tile):
        coef = jnp.dot(
            weights, table_ref[:, step * tile : (step + 1) * tile], preferred_element_type=F32
        )
        real, imag = coef[:atoms], coef[atoms:]
        cosine, sine = phase_ref[step, 0], phase_ref[step, 1]
        aug_ref[0:1, step * tile : (step + 1) * tile] = jnp.sum(real * cosine + imag * sine, axis=0, keepdims=True)
        aug_ref[1:2, step * tile : (step + 1) * tile] = jnp.sum(imag * cosine - real * sine, axis=0, keepdims=True)

    lines_ref[...] = jnp.zeros_like(lines_ref)
    half = lines_ref.shape[1] // 2
    aug = aug_ref[...]
    for t in range(slots):
        lines_ref[t : t + 1, 0:NZ] = aug[0:1, t * NZ : (t + 1) * NZ]
        lines_ref[t : t + 1, half : half + NZ] = aug[1:2, t * NZ : (t + 1) * NZ]
    high, low = split(lines_ref[...])
    spread_copy.wait()
    lane = lax.broadcasted_iota(jnp.int32, (slots, lanes), 1)
    slot = lax.broadcasted_iota(jnp.int32, (slots, lanes), 0)
    marks = jnp.zeros((slots, lanes), F32)
    for t in range(slots):
        marks = jnp.where(slot == t, columns_ref[t].astype(F32), marks)
    both = jnp.concatenate([high, low], axis=0)
    packed = jnp.dot(both, spread_ref[0], preferred_element_type=F32)
    packed = packed[:slots] + packed[slots:] + jnp.dot(high, spread_ref[1], preferred_element_type=F32)
    for g in range(groups):
        stick_ref[g] = jnp.where(lane == 2 * planes, marks, packed[:, g * lanes : (g + 1) * lanes])

    def stick_copy(step, slot):
        target = peer(step)
        return pltpu.make_async_remote_copy(
            src_ref=stick_ref.at[target[1]],
            dst_ref=out_ref.at[slot],
            send_sem=dev_send.at[step],
            recv_sem=dev_recv.at[slot],
            device_id=target,
            device_id_type=MESH,
        )

    @pl.loop(1, devices)
    def _(step):
        stick_copy(step, place).start()

    out_ref[place] = stick_ref[me]

    @pl.loop(1, devices)
    def _(step):
        stick_copy(step, lax.rem(place + step, devices)).wait_recv()

    for step in range(1, groups):
        target = lax.rem(me + step, groups)
        rs_copy(0, 0, target, me).wait_send()
        ga_copy(step, me).wait_send()
    for step in range(1, bands):
        band_copy(step, band).wait_send()

    @pl.loop(1, devices)
    def _(step):
        stick_copy(step, place).wait_send()


def finish_kernel(bands, groups, received_ref, out_ref, table_ref, turned_ref, angle_ref):
    total, lanes = received_ref.shape
    planes = out_ref.shape[0]
    y_block = out_ref.shape[1]
    y_pad = angle_ref.shape[1]
    band = lax.axis_index("band")
    received = received_ref[...]
    turned = jnp.swapaxes(received, 0, 1)
    turned_ref[...] = turned
    column_row = turned[2 * planes : 2 * planes + 1, :]
    live_row = column_row >= 0.0
    x_row = jnp.floor((column_row + 0.5) * (1.0 / NY))
    y_row = column_row - x_row * NY
    y_values = lax.broadcasted_iota(jnp.int32, (y_pad, total), 0) + band * y_block
    cos_y, sin_y = turn_cos_sin(y_values.astype(F32) * y_row, NY)
    angle_ref[0] = jnp.where(live_row, cos_y, 0.0)
    angle_ref[1] = jnp.where(live_row, sin_y, 0.0)
    column = received[:, 2 * planes : 2 * planes + 1]
    owner = lax.broadcasted_iota(jnp.int32, (total, 1), 0) // (total // bands)
    x = jnp.floor((column + 0.5) * (1.0 / NY)) + owner.astype(F32) * (NX // bands)
    x_values = lax.broadcasted_iota(jnp.int32, (total, 256), 1).astype(F32)
    cos_x, sin_x = turn_cos_sin(x * x_values, NX)
    for part, value in enumerate(split(cos_x)):
        table_ref[part, 0:total, 0:256] = value
        table_ref[part, total : 2 * total, 256:512] = value
    for part, value in enumerate(split(sin_x)):
        table_ref[part, 0:total, 256:512] = value
        table_ref[part, total : 2 * total, 0:256] = -value

    @pl.loop(0, planes)
    def _(z):
        real = turned_ref[pl.ds(z, 1), :]
        imag = turned_ref[pl.ds(planes + z, 1), :]
        cosine, sine = angle_ref[0], angle_ref[1]
        amp = jnp.concatenate([real * cosine - imag * sine, real * sine + imag * cosine], axis=1).astype(BF16)
        result = jnp.dot(amp, table_ref[0], preferred_element_type=F32)
        result = result + jnp.dot(amp, table_ref[1], preferred_element_type=F32)
        out_ref[z, :, 0, :] = result[:y_block, 0:NX]
        out_ref[z, :, 1, :] = result[:y_block, 256 : 256 + NX]


def on_device(
    waves, occupations, beta_table, wave_miller, atom_kinds, atom_sites, aug_table, stick_columns
):
    bands = lax.axis_size("band")
    groups = lax.axis_size("ga")
    devices = bands * groups
    atoms = atom_sites.shape[1]
    slots = stick_columns.shape[0]
    nb = waves.shape[1]
    width = waves.shape[2]
    points = aug_table.shape[1]
    planes = NZ // groups
    pairs = len(PAIR_FIRST)
    own = atoms // groups
    block = own * max(1, 32 // own)
    steps = atoms // block
    cols = 4 * nb
    tile = math.gcd(points, 256)
    lanes = up(2 * planes + 1, 128)
    chunks = 128 // own
    chunk = up(-(-pairs // chunks), 8)

    odd = (ELL[PAIR_FIRST] + ELL[PAIR_SECOND]) % 2 == 1
    factors = np.where(PAIR_FIRST == PAIR_SECOND, 1.0, 2.0)
    signs = np.stack([np.where(odd, 0.0, factors), np.where(odd, -factors, 0.0)], axis=1).astype(np.float32)
    angle = (np.outer(np.arange(NZ), np.arange(NZ)) % NZ) * (2.0 * np.pi / NZ)
    cos_z = np.cos(angle).reshape(NZ, groups, planes)
    sin_z = np.sin(angle).reshape(NZ, groups, planes)
    half = up(NZ, 128)
    spread = np.zeros((2 * half, groups, lanes), np.float32)
    spread[:NZ, :, :planes] = cos_z
    spread[half : half + NZ, :, :planes] = -sin_z
    spread[:NZ, :, planes : 2 * planes] = sin_z
    spread[half : half + NZ, :, planes : 2 * planes] = cos_z
    spread = spread.reshape(2 * half, groups * lanes)
    spread_high = spread.astype(BF16)
    spread_low = (spread - spread_high.astype(np.float32)).astype(BF16)
    vmem = pl.BlockSpec(memory_space=pltpu.VMEM)
    hbm = pl.BlockSpec(memory_space=pl.ANY)
    dma = pltpu.SemaphoreType.DMA
    part_lanes = up(NH * own, 128)
    received = pl.pallas_call(
        functools.partial(mega_kernel, bands, groups),
        in_specs=[vmem] * 6 + [pl.BlockSpec(memory_space=pltpu.SMEM), vmem, hbm, hbm],
        out_specs=vmem,
        out_shape=jax.ShapeDtypeStruct((devices, slots, lanes), F32),
        scratch_shapes=[
            pltpu.VMEM((8, atoms), F32),
            pltpu.VMEM((atoms, 8), F32),
            pltpu.VMEM((cols, 4 * width), BF16),
            pltpu.VMEM((HALF * block, 4 * width), BF16),
            pltpu.VMEM((steps, HALF, block, cols), F32),
            pltpu.VMEM((groups, HALF, own, cols), F32),
            pltpu.VMEM((points // tile, 2, atoms, tile), F32),
            pltpu.VMEM((up(HALF * own, 128), cols), F32),
            pltpu.VMEM((up(NH, 8), part_lanes), F32),
            pltpu.VMEM((bands, up(NH, 8), part_lanes), F32),
            pltpu.VMEM((chunk * chunks, own), F32),
            pltpu.VMEM((chunk, chunks * own), F32),
            pltpu.VMEM((groups, chunk, chunks * own), F32),
            pltpu.VMEM((up(SPECIES * pairs, 128), 2 * atoms), F32),
            pltpu.VMEM(aug_table.shape, BF16),
            pltpu.VMEM((2,) + spread.shape, BF16),
            pltpu.VMEM((8, points), F32),
            pltpu.VMEM((slots, 2 * half), F32),
            pltpu.VMEM((groups, slots, lanes), F32),
            dma((groups,)),
            dma((groups,)),
            dma((bands,)),
            dma((bands,)),
            dma((groups,)),
            dma((groups,)),
            dma((devices,)),
            dma((devices,)),
            dma((2,)),
        ],
        compiler_params=pltpu.CompilerParams(collective_id=0, has_side_effects=True),
        name="slots",
    )(
        waves,
        occupations[None, :],
        beta_table,
        wave_miller,
        atom_kinds[None, :],
        atom_sites,
        stick_columns,
        jnp.asarray(signs),
        aug_table,
        jnp.asarray(np.stack([spread_high, spread_low])),
    )
    y_block = NY // bands
    total = devices * slots
    result = pl.pallas_call(
        functools.partial(finish_kernel, bands, groups),
        in_specs=[vmem],
        out_specs=vmem,
        out_shape=jax.ShapeDtypeStruct((planes, y_block, 2, NX), F32),
        scratch_shapes=[
            pltpu.VMEM((2, 2 * total, 512), BF16),
            pltpu.VMEM((lanes, total), F32),
            pltpu.VMEM((2, up(y_block, 16), total), F32),
        ],
        name="finish",
    )(received.reshape(total, lanes))
    return result.transpose(2, 0, 1, 3)


def solution(mesh):
    in_specs = (
        P(None, "band", "ga"),
        P("band"),
        P(None, "ga"),
        P(None, "ga"),
        P(),
        P(),
        P(None, ("band", "ga")),
        P(("band", "ga")),
    )
    out_specs = P(None, "ga", "band", None)
    return jax.shard_map(
        on_device, mesh=mesh, in_specs=in_specs, out_specs=out_specs, check_vma=False
    )
```

```python
import functools
import math

import jax
import jax.numpy as jnp
import numpy as np
from jax import lax
from jax.experimental import pallas as pl
from jax.experimental.pallas import tpu as pltpu
from jax.sharding import PartitionSpec as P

NX = 240
NY = 240
NZ = 224
NH = 18
HALF = NH // 2
SPECIES = 4

PERIOD = math.lcm(NX, NY, NZ)
STEP_X = PERIOD // NX
STEP_Y = PERIOD // NY
STEP_Z = PERIOD // NZ
ELL = np.array([0, 0] + [1] * 6 + [2] * 10)
PAIR_FIRST, PAIR_SECOND = np.triu_indices(NH)

highest = lax.Precision.HIGHEST
F32 = jnp.float32
BF16 = jnp.bfloat16


def fit_even(func, terms):
    nodes = 0.125 * (1.0 + np.cos(np.pi * (np.arange(64) + 0.5) / 64))
    scaled = np.polynomial.chebyshev.Chebyshev.fit(nodes, func(np.sqrt(nodes)), terms - 1, domain=[0, 0.25])
    return [float(c) for c in scaled.convert(kind=np.polynomial.Polynomial).coef]


COS_FIT = fit_even(lambda u: np.cos(2 * np.pi * u), 7)
SIN_FIT = fit_even(lambda u: np.sin(2 * np.pi * u) / u, 6)


def horner(coefs, w):
    total = jnp.full_like(w, coefs[-1])
    for c in coefs[-2::-1]:
        total = total * w + c
    return total


def turn_cos_sin(count, period):
    rest = count - jnp.round(count * (1.0 / period)) * period
    u = rest * (1.0 / period)
    w = u * u
    return horner(COS_FIT, w), u * horner(SIN_FIT, w)


MESH = pl.DeviceIdType.MESH


def greet(peers, axis_sets):
    barrier = pltpu.get_barrier_semaphore()
    for count, device_of in axis_sets:

        @pl.loop(1, count)
        def _(step):
            pl.semaphore_signal(barrier, inc=1, device_id=device_of(step), device_id_type=MESH)

    pl.semaphore_wait(barrier, peers)


def up(value, unit):
    return -(-value // unit) * unit


def split(value):
    high = value.astype(BF16)
    return high, (value - high.astype(F32)).astype(BF16)


def mega_kernel(
    bands,
    groups,
    waves_ref,
    occ_ref,
    beta_ref,
    miller_ref,
    kinds_ref,
    site_ref,
    columns_ref,
    signs_ref,
    table_hbm,
    spread_hbm,
    out_ref,
    small_ref,
    site_t_ref,
    wave_ref,
    rows_ref,
    send_ref,
    recv_ref,
    phase_ref,
    total_ref,
    part_ref,
    band_ref,
    pair_ref,
    pack_ref,
    all_ref,
    weights_ref,
    table_ref,
    spread_ref,
    aug_ref,
    lines_ref,
    stick_ref,
    rs_send,
    rs_recv,
    band_send,
    band_recv,
    ga_send,
    ga_recv,
    dev_send,
    dev_recv,
    local_sem,
):
    band, me = lax.axis_index("band"), lax.axis_index("ga")
    devices = bands * groups
    place = band * groups + me
    atoms = site_ref.shape[1]
    own = atoms // groups
    width = miller_ref.shape[1]
    nb = waves_ref.shape[1]
    slots = columns_ref.shape[0]
    steps, _, block, cols = send_ref.shape
    ratio = block // own
    points = slots * NZ
    tile = phase_ref.shape[-1]
    planes = NZ // groups
    lanes = stick_ref.shape[-1]
    pairs = len(PAIR_FIRST)

    table_copy = pltpu.make_async_copy(table_hbm, table_ref, local_sem.at[0])
    spread_copy = pltpu.make_async_copy(spread_hbm, spread_ref, local_sem.at[1])
    table_copy.start()
    spread_copy.start()

    def peer(step):
        other = lax.rem(place + step, devices)
        return other // groups, lax.rem(other, groups)

    greet(devices - 1, [(devices, peer)])

    small_ref[...] = jnp.zeros_like(small_ref)
    small_ref[0:1, :] = site_ref[0:1, :].astype(F32) * STEP_X
    small_ref[1:2, :] = site_ref[1:2, :].astype(F32) * STEP_Y
    small_ref[2:3, :] = site_ref[2:3, :].astype(F32) * STEP_Z
    small_ref[3:4, :] = kinds_ref[...].astype(F32)
    small_ref[4:5, 0:nb] = occ_ref[...]
    small_ref[4:5, nb : 2 * nb] = occ_ref[...]
    site_t_ref[...] = jnp.swapaxes(small_ref[...], 0, 1)

    wave_ref[...] = jnp.zeros_like(wave_ref)
    re, im = waves_ref[0], waves_ref[1]
    for h in range(2):
        r, c = 2 * nb * h, 2 * width * h
        wave_ref[r : r + nb, c : c + width] = re
        wave_ref[r : r + nb, c + width : c + 2 * width] = im
        wave_ref[r + nb : r + 2 * nb, c : c + width] = im
        wave_ref[r + nb : r + 2 * nb, c + width : c + 2 * width] = -re

    def rs_copy(index, part, target, slot):
        return pltpu.make_async_remote_copy(
            src_ref=send_ref.at[index, :, pl.ds(pl.multiple_of(part * own, own), own), :],
            dst_ref=recv_ref.at[slot],
            send_sem=rs_send.at[target],
            recv_sem=rs_recv.at[slot],
            device_id=(band, target),
            device_id_type=MESH,
        )

    @pl.loop(0, steps)
    def _(step):
        index = lax.rem(me // ratio + 1 + step, steps)
        start = pl.multiple_of(index * block, block)
        site = site_t_ref[pl.ds(start, block), :]
        kinds = site[:, 3:4]
        miller = miller_ref[...].astype(F32)
        count = site[:, 0:1] * miller[0:1, :] + site[:, 1:2] * miller[1:2, :] + site[:, 2:3] * miller[2:3, :]
        cosine, sine = turn_cos_sin(count, PERIOD)
        masks = [kinds == float(s) for s in range(1, SPECIES)]
        for i in range(NH):
            radial = jnp.broadcast_to(beta_ref[i : i + 1, :], (block, width))
            for s in range(1, SPECIES):
                radial = jnp.where(masks[s - 1], beta_ref[s * NH + i : s * NH + i + 1, :], radial)
            if ELL[i] == 0:
                real, imag = radial * cosine, -(radial * sine)
            elif ELL[i] == 1:
                real, imag = -(radial * sine), -(radial * cosine)
            else:
                real, imag = -(radial * cosine), radial * sine
            row = (i % HALF) * block
            col = (i // HALF) * 2 * width
            rows_ref[row : row + block, col : col + width] = real.astype(BF16)
            rows_ref[row : row + block, col + width : col + 2 * width] = imag.astype(BF16)
        result = lax.dot_general(
            rows_ref[...], wave_ref[...], (((1,), (1,)), ((), ())), preferred_element_type=F32
        )
        send_ref[index] = result.reshape(HALF, block, cols)
        for part in range(ratio):
            target = index * ratio + part

            @pl.when(target != me)
            def _():
                rs_copy(index, part, target, me).start()

    @pl.loop(0, points // tile)
    def _(step):
        point = step * tile + lax.broadcasted_iota(jnp.int32, (1, tile), 1)
        x_row = jnp.zeros((1, tile), F32)
        y_row = jnp.zeros((1, tile), F32)
        z_row = point.astype(F32)
        for t in range(slots):
            column = columns_ref[t]
            x = band * (NX // bands) + lax.div(column, NY)
            y = lax.rem(column, NY)
            inside = point >= t * NZ
            x_row = jnp.where(inside, x.astype(F32), x_row)
            y_row = jnp.where(inside, y.astype(F32), y_row)
            z_row = jnp.where(inside, (point - t * NZ).astype(F32), z_row)
        count = site_t_ref[:, 0:1] * x_row + site_t_ref[:, 1:2] * y_row + site_t_ref[:, 2:3] * z_row
        cosine, sine = turn_cos_sin(count, PERIOD)
        phase_ref[step, 0] = cosine
        phase_ref[step, 1] = sine

    total = send_ref[me // ratio, :, pl.ds(pl.multiple_of(lax.rem(me, ratio) * own, own), own), :]
    for step in range(1, groups):
        source = lax.rem(me + step, groups)
        rs_copy(0, 0, source, source).wait_recv()
        total = total + recv_ref[source]

    total_ref[...] = jnp.zeros_like(total_ref)
    total_ref[0 : HALF * own, :] = total.reshape(HALF * own, cols)
    turned = jnp.swapaxes(total_ref[...], 0, 1)
    becp = jnp.concatenate([turned[0 : 2 * nb, : HALF * own], turned[2 * nb :, : HALF * own]], axis=1)
    scaled = becp * site_t_ref[0 : 2 * nb, 4:5]
    part_ref[...] = jnp.zeros_like(part_ref)
    for d in range(NH):
        size = (NH - d) * own
        product = scaled[:, :size] * becp[:, d * own :]
        part_ref[d : d + 1, 0:size] = jnp.sum(product, axis=0, keepdims=True)

    def band_copy(step, slot):
        return pltpu.make_async_remote_copy(
            src_ref=part_ref,
            dst_ref=band_ref.at[slot],
            send_sem=band_send.at[step],
            recv_sem=band_recv.at[slot],
            device_id=(lax.rem(band + step, bands), me),
            device_id_type=MESH,
        )

    for step in range(1, bands):
        band_copy(step, band).start()
    band_ref[band] = part_ref[...]
    for step in range(1, bands):
        band_copy(step, lax.rem(band + step, bands)).wait_recv()
    summed = band_ref[0]
    for source in range(1, bands):
        summed = summed + band_ref[source]

    pair_ref[...] = jnp.zeros_like(pair_ref)
    begin = 0
    for i in range(NH):
        pair_ref[begin : begin + NH - i, :] = summed[: NH - i, i * own : (i + 1) * own]
        begin += NH - i
    chunk = pack_ref.shape[0]
    chunks = pack_ref.shape[1] // own
    pack_ref[...] = jnp.concatenate(
        [pair_ref[q * chunk : (q + 1) * chunk, :] for q in range(chunks)], axis=1
    )

    def ga_copy(step, slot):
        return pltpu.make_async_remote_copy(
            src_ref=pack_ref,
            dst_ref=all_ref.at[slot],
            send_sem=ga_send.at[step],
            recv_sem=ga_recv.at[slot],
            device_id=(band, lax.rem(me + step, groups)),
            device_id_type=MESH,
        )

    for step in range(1, groups):
        ga_copy(step, me).start()
    all_ref[me] = pack_ref[...]
    for step in range(1, groups):
        ga_copy(step, lax.rem(me + step, groups)).wait_recv()
    becsum = jnp.concatenate(
        [
            jnp.concatenate([all_ref[g, :, q * own : (q + 1) * own] for g in range(groups)], axis=1)
            for q in range(chunks)
        ],
        axis=0,
    )[:pairs]
    even = becsum * signs_ref[:, 0:1]
    odd = becsum * signs_ref[:, 1:2]
    kind_row = small_ref[3:4, :]
    weights_ref[...] = jnp.zeros_like(weights_ref)
    for s in range(SPECIES):
        here = kind_row == float(s)
        weights_ref[s * pairs : (s + 1) * pairs, 0:atoms] = jnp.where(here, even, 0.0)
        weights_ref[s * pairs : (s + 1) * pairs, atoms : 2 * atoms] = jnp.where(here, odd, 0.0)
    weights = jnp.swapaxes(weights_ref[...], 0, 1).astype(BF16)[:, : SPECIES * pairs]

    table_copy.wait()
    for step in range(points // tile):
        coef = jnp.dot(
            weights, table_ref[:, step * tile : (step + 1) * tile], preferred_element_type=F32
        )
        real, imag = coef[:atoms], coef[atoms:]
        cosine, sine = phase_ref[step, 0], phase_ref[step, 1]
        aug_ref[0:1, step * tile : (step + 1) * tile] = jnp.sum(real * cosine + imag * sine, axis=0, keepdims=True)
        aug_ref[1:2, step * tile : (step + 1) * tile] = jnp.sum(imag * cosine - real * sine, axis=0, keepdims=True)

    lines_ref[...] = jnp.zeros_like(lines_ref)
    half = lines_ref.shape[1] // 2
    aug = aug_ref[...]
    for t in range(slots):
        lines_ref[t : t + 1, 0:NZ] = aug[0:1, t * NZ : (t + 1) * NZ]
        lines_ref[t : t + 1, half : half + NZ] = aug[1:2, t * NZ : (t + 1) * NZ]
    high, low = split(lines_ref[...])
    spread_copy.wait()
    lane = lax.broadcasted_iota(jnp.int32, (slots, lanes), 1)
    slot = lax.broadcasted_iota(jnp.int32, (slots, lanes), 0)
    marks = jnp.zeros((slots, lanes), F32)
    for t in range(slots):
        marks = jnp.where(slot == t, columns_ref[t].astype(F32), marks)
    both = jnp.concatenate([high, low], axis=0)
    packed = jnp.dot(both, spread_ref[0], preferred_element_type=F32)
    packed = packed[:slots] + packed[slots:] + jnp.dot(high, spread_ref[1], preferred_element_type=F32)
    for g in range(groups):
        stick_ref[g] = jnp.where(lane == 2 * planes, marks, packed[:, g * lanes : (g + 1) * lanes])

    def stick_copy(step, slot):
        target = peer(step)
        return pltpu.make_async_remote_copy(
            src_ref=stick_ref.at[target[1]],
            dst_ref=out_ref.at[slot],
            send_sem=dev_send.at[step],
            recv_sem=dev_recv.at[slot],
            device_id=target,
            device_id_type=MESH,
        )

    @pl.loop(1, devices)
    def _(step):
        stick_copy(step, place).start()

    out_ref[place] = stick_ref[me]

    @pl.loop(1, devices)
    def _(step):
        stick_copy(step, lax.rem(place + step, devices)).wait_recv()

    for step in range(1, groups):
        target = lax.rem(me + step, groups)
        rs_copy(0, 0, target, me).wait_send()
        ga_copy(step, me).wait_send()
    for step in range(1, bands):
        band_copy(step, band).wait_send()

    @pl.loop(1, devices)
    def _(step):
        stick_copy(step, place).wait_send()


def finish_kernel(bands, planes, received_ref, out_ref, table_ref, turned_ref, angle_ref, amp_ref):
    total, lanes = received_ref.shape
    batch = out_ref.shape[0]
    y_block = out_ref.shape[1]
    y_pad = angle_ref.shape[1]
    band = lax.axis_index("band")
    group = pl.program_id(0)

    @pl.when(group == 0)
    def _():
        received = received_ref[...]
        turned = jnp.swapaxes(received, 0, 1)
        turned_ref[...] = turned
        column_row = turned[2 * planes : 2 * planes + 1, :]
        live_row = column_row >= 0.0
        x_row = jnp.floor((column_row + 0.5) * (1.0 / NY))
        y_row = column_row - x_row * NY
        y_values = lax.broadcasted_iota(jnp.int32, (y_pad, total), 0) + band * y_block
        cos_y, sin_y = turn_cos_sin(y_values.astype(F32) * y_row, NY)
        angle_ref[0] = jnp.where(live_row, cos_y, 0.0)
        angle_ref[1] = jnp.where(live_row, sin_y, 0.0)
        column = received[:, 2 * planes : 2 * planes + 1]
        owner = lax.broadcasted_iota(jnp.int32, (total, 1), 0) // (total // bands)
        x = jnp.floor((column + 0.5) * (1.0 / NY)) + owner.astype(F32) * (NX // bands)
        x_values = lax.broadcasted_iota(jnp.int32, (total, 256), 1).astype(F32)
        cos_x, sin_x = turn_cos_sin(x * x_values, NX)
        for part, value in enumerate(split(cos_x)):
            table_ref[part, 0:total, 0:256] = value
            table_ref[part, total : 2 * total, 256:512] = value
        for part, value in enumerate(split(sin_x)):
            table_ref[part, 0:total, 256:512] = value
            table_ref[part, total : 2 * total, 0:256] = -value

    for k in range(batch):
        real = turned_ref[pl.ds(group * batch + k, 1), :]
        imag = turned_ref[pl.ds(planes + group * batch + k, 1), :]
        cosine, sine = angle_ref[0], angle_ref[1]
        row = k * y_pad
        amp_ref[row : row + y_pad, 0:total] = (real * cosine - imag * sine).astype(BF16)
        amp_ref[row : row + y_pad, total : 2 * total] = (real * sine + imag * cosine).astype(BF16)
    amp = amp_ref[...]
    for part in range(2):
        lane = slice(256 * part, 256 * part + 256)
        result = jnp.dot(amp, table_ref[0, :, lane], preferred_element_type=F32)
        result = result + jnp.dot(amp, table_ref[1, :, lane], preferred_element_type=F32)
        for k in range(batch):
            out_ref[k, :, part, :] = result[k * y_pad : k * y_pad + y_block, 0:NX]


def on_device(
    waves, occupations, beta_table, wave_miller, atom_kinds, atom_sites, aug_table, stick_columns
):
    bands = lax.axis_size("band")
    groups = lax.axis_size("ga")
    devices = bands * groups
    atoms = atom_sites.shape[1]
    slots = stick_columns.shape[0]
    nb = waves.shape[1]
    width = waves.shape[2]
    points = aug_table.shape[1]
    planes = NZ // groups
    pairs = len(PAIR_FIRST)
    own = atoms // groups
    block = own * max(1, 32 // own)
    steps = atoms // block
    cols = 4 * nb
    tile = math.gcd(points, 256)
    lanes = up(2 * planes + 1, 128)
    chunks = 128 // own
    chunk = up(-(-pairs // chunks), 8)

    odd = (ELL[PAIR_FIRST] + ELL[PAIR_SECOND]) % 2 == 1
    factors = np.where(PAIR_FIRST == PAIR_SECOND, 1.0, 2.0)
    signs = np.stack([np.where(odd, 0.0, factors), np.where(odd, -factors, 0.0)], axis=1).astype(np.float32)
    angle = (np.outer(np.arange(NZ), np.arange(NZ)) % NZ) * (2.0 * np.pi / NZ)
    cos_z = np.cos(angle).reshape(NZ, groups, planes)
    sin_z = np.sin(angle).reshape(NZ, groups, planes)
    half = up(NZ, 128)
    spread = np.zeros((2 * half, groups, lanes), np.float32)
    spread[:NZ, :, :planes] = cos_z
    spread[half : half + NZ, :, :planes] = -sin_z
    spread[:NZ, :, planes : 2 * planes] = sin_z
    spread[half : half + NZ, :, planes : 2 * planes] = cos_z
    spread = spread.reshape(2 * half, groups * lanes)
    spread_high = spread.astype(BF16)
    spread_low = (spread - spread_high.astype(np.float32)).astype(BF16)
    vmem = pl.BlockSpec(memory_space=pltpu.VMEM)
    hbm = pl.BlockSpec(memory_space=pl.ANY)
    dma = pltpu.SemaphoreType.DMA
    part_lanes = up(NH * own, 128)
    received = pl.pallas_call(
        functools.partial(mega_kernel, bands, groups),
        in_specs=[vmem] * 6 + [pl.BlockSpec(memory_space=pltpu.SMEM), vmem, hbm, hbm],
        out_specs=vmem,
        out_shape=jax.ShapeDtypeStruct((devices, slots, lanes), F32),
        scratch_shapes=[
            pltpu.VMEM((8, atoms), F32),
            pltpu.VMEM((atoms, 8), F32),
            pltpu.VMEM((cols, 4 * width), BF16),
            pltpu.VMEM((HALF * block, 4 * width), BF16),
            pltpu.VMEM((steps, HALF, block, cols), F32),
            pltpu.VMEM((groups, HALF, own, cols), F32),
            pltpu.VMEM((points // tile, 2, atoms, tile), F32),
            pltpu.VMEM((up(HALF * own, 128), cols), F32),
            pltpu.VMEM((up(NH, 8), part_lanes), F32),
            pltpu.VMEM((bands, up(NH, 8), part_lanes), F32),
            pltpu.VMEM((chunk * chunks, own), F32),
            pltpu.VMEM((chunk, chunks * own), F32),
            pltpu.VMEM((groups, chunk, chunks * own), F32),
            pltpu.VMEM((up(SPECIES * pairs, 128), 2 * atoms), F32),
            pltpu.VMEM(aug_table.shape, BF16),
            pltpu.VMEM((2,) + spread.shape, BF16),
            pltpu.VMEM((8, points), F32),
            pltpu.VMEM((slots, 2 * half), F32),
            pltpu.VMEM((groups, slots, lanes), F32),
            dma((groups,)),
            dma((groups,)),
            dma((bands,)),
            dma((bands,)),
            dma((groups,)),
            dma((groups,)),
            dma((devices,)),
            dma((devices,)),
            dma((2,)),
        ],
        compiler_params=pltpu.CompilerParams(collective_id=0, has_side_effects=True),
        name="slots",
    )(
        waves,
        occupations[None, :],
        beta_table,
        wave_miller,
        atom_kinds[None, :],
        atom_sites,
        stick_columns,
        jnp.asarray(signs),
        aug_table,
        jnp.asarray(np.stack([spread_high, spread_low])),
    )
    y_block = NY // bands
    total = devices * slots
    batch = math.gcd(planes, 7)
    y_pad = up(y_block, 16)
    result = pl.pallas_call(
        functools.partial(finish_kernel, bands, planes),
        grid=(planes // batch,),
        in_specs=[pl.BlockSpec((total, lanes), lambda g: (0, 0))],
        out_specs=pl.BlockSpec((batch, y_block, 2, NX), lambda g: (g, 0, 0, 0)),
        out_shape=jax.ShapeDtypeStruct((planes, y_block, 2, NX), F32),
        scratch_shapes=[
            pltpu.VMEM((2, 2 * total, 512), BF16),
            pltpu.VMEM((lanes, total), F32),
            pltpu.VMEM((2, y_pad, total), F32),
            pltpu.VMEM((batch * y_pad, 2 * total), BF16),
        ],
        name="finish",
    )(received.reshape(total, lanes))
    return result.transpose(2, 0, 1, 3)


def solution(mesh):
    in_specs = (
        P(None, "band", "ga"),
        P("band"),
        P(None, "ga"),
        P(None, "ga"),
        P(),
        P(),
        P(None, ("band", "ga")),
        P(("band", "ga")),
    )
    out_specs = P(None, "ga", "band", None)
    return jax.shard_map(
        on_device, mesh=mesh, in_specs=in_specs, out_specs=out_specs, check_vma=False
    )
```

```python
import functools
import math

import jax
import jax.numpy as jnp
import numpy as np
from jax import lax
from jax.experimental import pallas as pl
from jax.experimental.pallas import tpu as pltpu
from jax.sharding import PartitionSpec as P

NX = 240
NY = 240
NZ = 224
NH = 18
HALF = NH // 2
SPECIES = 4

PERIOD = math.lcm(NX, NY, NZ)
STEP_X = PERIOD // NX
STEP_Y = PERIOD // NY
STEP_Z = PERIOD // NZ
ELL = np.array([0, 0] + [1] * 6 + [2] * 10)
PAIR_FIRST, PAIR_SECOND = np.triu_indices(NH)

highest = lax.Precision.HIGHEST
F32 = jnp.float32
BF16 = jnp.bfloat16


def fit_even(func, terms):
    nodes = 0.125 * (1.0 + np.cos(np.pi * (np.arange(64) + 0.5) / 64))
    scaled = np.polynomial.chebyshev.Chebyshev.fit(nodes, func(np.sqrt(nodes)), terms - 1, domain=[0, 0.25])
    return [float(c) for c in scaled.convert(kind=np.polynomial.Polynomial).coef]


COS_FIT = fit_even(lambda u: np.cos(2 * np.pi * u), 7)
SIN_FIT = fit_even(lambda u: np.sin(2 * np.pi * u) / u, 6)


def horner(coefs, w):
    total = jnp.full_like(w, coefs[-1])
    for c in coefs[-2::-1]:
        total = total * w + c
    return total


def turn_cos_sin(count, period):
    rest = count - jnp.round(count * (1.0 / period)) * period
    u = rest * (1.0 / period)
    w = u * u
    return horner(COS_FIT, w), u * horner(SIN_FIT, w)


MESH = pl.DeviceIdType.MESH


def greet(peers, axis_sets):
    barrier = pltpu.get_barrier_semaphore()
    for count, device_of in axis_sets:

        @pl.loop(1, count)
        def _(step):
            pl.semaphore_signal(barrier, inc=1, device_id=device_of(step), device_id_type=MESH)

    return lambda: pl.semaphore_wait(barrier, peers)


def up(value, unit):
    return -(-value // unit) * unit


def split(value):
    high = value.astype(BF16)
    return high, (value - high.astype(F32)).astype(BF16)


def mega_kernel(
    bands,
    groups,
    waves_ref,
    occ_ref,
    beta_ref,
    miller_ref,
    kinds_ref,
    site_ref,
    columns_ref,
    signs_ref,
    table_hbm,
    spread_hbm,
    out_ref,
    small_ref,
    site_t_ref,
    wave_ref,
    rows_ref,
    send_ref,
    recv_ref,
    phase_ref,
    total_ref,
    part_ref,
    band_ref,
    pair_ref,
    pack_ref,
    all_ref,
    weights_ref,
    table_ref,
    spread_ref,
    aug_ref,
    lines_ref,
    stick_ref,
    rs_send,
    rs_recv,
    band_send,
    band_recv,
    ga_send,
    ga_recv,
    dev_send,
    dev_recv,
    local_sem,
):
    band, me = lax.axis_index("band"), lax.axis_index("ga")
    devices = bands * groups
    place = band * groups + me
    atoms = site_ref.shape[1]
    own = atoms // groups
    width = miller_ref.shape[1]
    nb = waves_ref.shape[1]
    slots = columns_ref.shape[0]
    steps, _, block, cols = send_ref.shape
    ratio = block // own
    points = slots * NZ
    tile = phase_ref.shape[-1]
    planes = NZ // groups
    lanes = stick_ref.shape[-1]
    pairs = len(PAIR_FIRST)

    table_copy = pltpu.make_async_copy(table_hbm, table_ref, local_sem.at[0])
    spread_copy = pltpu.make_async_copy(spread_hbm, spread_ref, local_sem.at[1])
    table_copy.start()
    spread_copy.start()

    def peer(step):
        other = lax.rem(place + step, devices)
        return other // groups, lax.rem(other, groups)

    all_here = greet(devices - 1, [(devices, peer)])

    small_ref[...] = jnp.zeros_like(small_ref)
    small_ref[0:1, :] = site_ref[0:1, :].astype(F32) * STEP_X
    small_ref[1:2, :] = site_ref[1:2, :].astype(F32) * STEP_Y
    small_ref[2:3, :] = site_ref[2:3, :].astype(F32) * STEP_Z
    small_ref[3:4, :] = kinds_ref[...].astype(F32)
    small_ref[4:5, 0:nb] = occ_ref[...]
    small_ref[4:5, nb : 2 * nb] = occ_ref[...]
    site_t_ref[...] = jnp.swapaxes(small_ref[...], 0, 1)

    wave_ref[...] = jnp.zeros_like(wave_ref)
    re, im = waves_ref[0], waves_ref[1]
    for h in range(2):
        r, c = 2 * nb * h, 2 * width * h
        wave_ref[r : r + nb, c : c + width] = re
        wave_ref[r : r + nb, c + width : c + 2 * width] = im
        wave_ref[r + nb : r + 2 * nb, c : c + width] = im
        wave_ref[r + nb : r + 2 * nb, c + width : c + 2 * width] = -re

    def rs_copy(index, part, target, slot):
        return pltpu.make_async_remote_copy(
            src_ref=send_ref.at[index, :, pl.ds(pl.multiple_of(part * own, own), own), :],
            dst_ref=recv_ref.at[slot],
            send_sem=rs_send.at[target],
            recv_sem=rs_recv.at[slot],
            device_id=(band, target),
            device_id_type=MESH,
        )

    @pl.loop(0, steps)
    def _(step):
        index = lax.rem(me // ratio + 1 + step, steps)
        start = pl.multiple_of(index * block, block)
        site = site_t_ref[pl.ds(start, block), :]
        kinds = site[:, 3:4]
        miller = miller_ref[...].astype(F32)
        count = site[:, 0:1] * miller[0:1, :] + site[:, 1:2] * miller[1:2, :] + site[:, 2:3] * miller[2:3, :]
        cosine, sine = turn_cos_sin(count, PERIOD)
        masks = [kinds == float(s) for s in range(1, SPECIES)]
        for i in range(NH):
            radial = jnp.broadcast_to(beta_ref[i : i + 1, :], (block, width))
            for s in range(1, SPECIES):
                radial = jnp.where(masks[s - 1], beta_ref[s * NH + i : s * NH + i + 1, :], radial)
            if ELL[i] == 0:
                real, imag = radial * cosine, -(radial * sine)
            elif ELL[i] == 1:
                real, imag = -(radial * sine), -(radial * cosine)
            else:
                real, imag = -(radial * cosine), radial * sine
            row = (i % HALF) * block
            col = (i // HALF) * 2 * width
            rows_ref[row : row + block, col : col + width] = real.astype(BF16)
            rows_ref[row : row + block, col + width : col + 2 * width] = imag.astype(BF16)
        result = lax.dot_general(
            rows_ref[...], wave_ref[...], (((1,), (1,)), ((), ())), preferred_element_type=F32
        )
        send_ref[index] = result.reshape(HALF, block, cols)

        @pl.when(step == 0)
        def _():
            all_here()

        for part in range(ratio):
            target = index * ratio + part

            @pl.when(target != me)
            def _():
                rs_copy(index, part, target, me).start()

    @pl.loop(0, points // tile)
    def _(step):
        point = step * tile + lax.broadcasted_iota(jnp.int32, (1, tile), 1)
        x_row = jnp.zeros((1, tile), F32)
        y_row = jnp.zeros((1, tile), F32)
        z_row = point.astype(F32)
        for t in range(slots):
            column = columns_ref[t]
            x = band * (NX // bands) + lax.div(column, NY)
            y = lax.rem(column, NY)
            inside = point >= t * NZ
            x_row = jnp.where(inside, x.astype(F32), x_row)
            y_row = jnp.where(inside, y.astype(F32), y_row)
            z_row = jnp.where(inside, (point - t * NZ).astype(F32), z_row)
        count = site_t_ref[:, 0:1] * x_row + site_t_ref[:, 1:2] * y_row + site_t_ref[:, 2:3] * z_row
        cosine, sine = turn_cos_sin(count, PERIOD)
        phase_ref[step, 0] = cosine
        phase_ref[step, 1] = sine

    total = send_ref[me // ratio, :, pl.ds(pl.multiple_of(lax.rem(me, ratio) * own, own), own), :]
    for step in range(1, groups):
        source = lax.rem(me + step, groups)
        rs_copy(0, 0, source, source).wait_recv()
        total = total + recv_ref[source]

    total_ref[...] = jnp.zeros_like(total_ref)
    total_ref[0 : HALF * own, :] = total.reshape(HALF * own, cols)
    turned = jnp.swapaxes(total_ref[...], 0, 1)
    becp = jnp.concatenate([turned[0 : 2 * nb, : HALF * own], turned[2 * nb :, : HALF * own]], axis=1)
    scaled = becp * site_t_ref[0 : 2 * nb, 4:5]
    part_ref[...] = jnp.zeros_like(part_ref)
    for d in range(NH):
        size = (NH - d) * own
        product = scaled[:, :size] * becp[:, d * own :]
        part_ref[d : d + 1, 0:size] = jnp.sum(product, axis=0, keepdims=True)

    def band_copy(step, slot):
        return pltpu.make_async_remote_copy(
            src_ref=part_ref,
            dst_ref=band_ref.at[slot],
            send_sem=band_send.at[step],
            recv_sem=band_recv.at[slot],
            device_id=(lax.rem(band + step, bands), me),
            device_id_type=MESH,
        )

    for step in range(1, bands):
        band_copy(step, band).start()
    band_ref[band] = part_ref[...]
    for step in range(1, bands):
        band_copy(step, lax.rem(band + step, bands)).wait_recv()
    summed = band_ref[0]
    for source in range(1, bands):
        summed = summed + band_ref[source]

    pair_ref[...] = jnp.zeros_like(pair_ref)
    begin = 0
    for i in range(NH):
        pair_ref[begin : begin + NH - i, :] = summed[: NH - i, i * own : (i + 1) * own]
        begin += NH - i
    chunk = pack_ref.shape[0]
    chunks = pack_ref.shape[1] // own
    pack_ref[...] = jnp.concatenate(
        [pair_ref[q * chunk : (q + 1) * chunk, :] for q in range(chunks)], axis=1
    )

    def ga_copy(step, slot):
        return pltpu.make_async_remote_copy(
            src_ref=pack_ref,
            dst_ref=all_ref.at[slot],
            send_sem=ga_send.at[step],
            recv_sem=ga_recv.at[slot],
            device_id=(band, lax.rem(me + step, groups)),
            device_id_type=MESH,
        )

    for step in range(1, groups):
        ga_copy(step, me).start()
    all_ref[me] = pack_ref[...]
    for step in range(1, groups):
        ga_copy(step, lax.rem(me + step, groups)).wait_recv()
    becsum = jnp.concatenate(
        [
            jnp.concatenate([all_ref[g, :, q * own : (q + 1) * own] for g in range(groups)], axis=1)
            for q in range(chunks)
        ],
        axis=0,
    )[:pairs]
    even = becsum * signs_ref[:, 0:1]
    odd = becsum * signs_ref[:, 1:2]
    kind_row = small_ref[3:4, :]
    weights_ref[...] = jnp.zeros_like(weights_ref)
    for s in range(SPECIES):
        here = kind_row == float(s)
        weights_ref[s * pairs : (s + 1) * pairs, 0:atoms] = jnp.where(here, even, 0.0)
        weights_ref[s * pairs : (s + 1) * pairs, atoms : 2 * atoms] = jnp.where(here, odd, 0.0)
    weights = jnp.swapaxes(weights_ref[...], 0, 1).astype(BF16)[:, : SPECIES * pairs]

    table_copy.wait()
    for step in range(points // tile):
        coef = jnp.dot(
            weights, table_ref[:, step * tile : (step + 1) * tile], preferred_element_type=F32
        )
        real, imag = coef[:atoms], coef[atoms:]
        cosine, sine = phase_ref[step, 0], phase_ref[step, 1]
        aug_ref[0:1, step * tile : (step + 1) * tile] = jnp.sum(real * cosine + imag * sine, axis=0, keepdims=True)
        aug_ref[1:2, step * tile : (step + 1) * tile] = jnp.sum(imag * cosine - real * sine, axis=0, keepdims=True)

    lines_ref[...] = jnp.zeros_like(lines_ref)
    half = lines_ref.shape[1] // 2
    aug = aug_ref[...]
    for t in range(slots):
        lines_ref[t : t + 1, 0:NZ] = aug[0:1, t * NZ : (t + 1) * NZ]
        lines_ref[t : t + 1, half : half + NZ] = aug[1:2, t * NZ : (t + 1) * NZ]
    high, low = split(lines_ref[...])
    spread_copy.wait()
    lane = lax.broadcasted_iota(jnp.int32, (slots, lanes), 1)
    slot = lax.broadcasted_iota(jnp.int32, (slots, lanes), 0)
    marks = jnp.zeros((slots, lanes), F32)
    for t in range(slots):
        marks = jnp.where(slot == t, columns_ref[t].astype(F32), marks)
    both = jnp.concatenate([high, low], axis=0)
    packed = jnp.dot(both, spread_ref[0], preferred_element_type=F32)
    packed = packed[:slots] + packed[slots:] + jnp.dot(high, spread_ref[1], preferred_element_type=F32)
    for g in range(groups):
        stick_ref[g] = jnp.where(lane == 2 * planes, marks, packed[:, g * lanes : (g + 1) * lanes])

    def stick_copy(step, slot):
        target = peer(step)
        return pltpu.make_async_remote_copy(
            src_ref=stick_ref.at[target[1]],
            dst_ref=out_ref.at[slot],
            send_sem=dev_send.at[step],
            recv_sem=dev_recv.at[slot],
            device_id=target,
            device_id_type=MESH,
        )

    @pl.loop(1, devices)
    def _(step):
        stick_copy(step, place).start()

    out_ref[place] = stick_ref[me]

    @pl.loop(1, devices)
    def _(step):
        stick_copy(step, lax.rem(place + step, devices)).wait_recv()

    for step in range(1, groups):
        target = lax.rem(me + step, groups)
        rs_copy(0, 0, target, me).wait_send()
        ga_copy(step, me).wait_send()
    for step in range(1, bands):
        band_copy(step, band).wait_send()

    @pl.loop(1, devices)
    def _(step):
        stick_copy(step, place).wait_send()


def finish_kernel(bands, planes, received_ref, out_ref, table_ref, turned_ref, angle_ref, amp_ref):
    total, lanes = received_ref.shape
    batch = out_ref.shape[0]
    y_block = out_ref.shape[1]
    y_pad = angle_ref.shape[1]
    band = lax.axis_index("band")
    group = pl.program_id(0)

    @pl.when(group == 0)
    def _():
        received = received_ref[...]
        turned = jnp.swapaxes(received, 0, 1)
        turned_ref[...] = turned
        column_row = turned[2 * planes : 2 * planes + 1, :]
        live_row = column_row >= 0.0
        x_row = jnp.floor((column_row + 0.5) * (1.0 / NY))
        y_row = column_row - x_row * NY
        y_values = lax.broadcasted_iota(jnp.int32, (y_pad, total), 0) + band * y_block
        cos_y, sin_y = turn_cos_sin(y_values.astype(F32) * y_row, NY)
        angle_ref[0] = jnp.where(live_row, cos_y, 0.0)
        angle_ref[1] = jnp.where(live_row, sin_y, 0.0)
        column = received[:, 2 * planes : 2 * planes + 1]
        owner = lax.broadcasted_iota(jnp.int32, (total, 1), 0) // (total // bands)
        x = jnp.floor((column + 0.5) * (1.0 / NY)) + owner.astype(F32) * (NX // bands)
        x_values = lax.broadcasted_iota(jnp.int32, (total, 256), 1).astype(F32)
        cos_x, sin_x = turn_cos_sin(x * x_values, NX)
        for part, value in enumerate(split(cos_x)):
            table_ref[part, 0:total, 0:256] = value
            table_ref[part, total : 2 * total, 256:512] = value
        for part, value in enumerate(split(sin_x)):
            table_ref[part, 0:total, 256:512] = value
            table_ref[part, total : 2 * total, 0:256] = -value

    for k in range(batch):
        real = turned_ref[pl.ds(group * batch + k, 1), :]
        imag = turned_ref[pl.ds(planes + group * batch + k, 1), :]
        cosine, sine = angle_ref[0], angle_ref[1]
        row = k * y_pad
        amp_ref[row : row + y_pad, 0:total] = (real * cosine - imag * sine).astype(BF16)
        amp_ref[row : row + y_pad, total : 2 * total] = (real * sine + imag * cosine).astype(BF16)
    amp = amp_ref[...]
    for part in range(2):
        lane = slice(256 * part, 256 * part + 256)
        result = jnp.dot(amp, table_ref[0, :, lane], preferred_element_type=F32)
        result = result + jnp.dot(amp, table_ref[1, :, lane], preferred_element_type=F32)
        for k in range(batch):
            out_ref[k, :, part, :] = result[k * y_pad : k * y_pad + y_block, 0:NX]


def on_device(
    waves, occupations, beta_table, wave_miller, atom_kinds, atom_sites, aug_table, stick_columns
):
    bands = lax.axis_size("band")
    groups = lax.axis_size("ga")
    devices = bands * groups
    atoms = atom_sites.shape[1]
    slots = stick_columns.shape[0]
    nb = waves.shape[1]
    width = waves.shape[2]
    points = aug_table.shape[1]
    planes = NZ // groups
    pairs = len(PAIR_FIRST)
    own = atoms // groups
    block = own * max(1, 32 // own)
    steps = atoms // block
    cols = 4 * nb
    tile = math.gcd(points, 256)
    lanes = up(2 * planes + 1, 128)
    chunks = 128 // own
    chunk = up(-(-pairs // chunks), 8)

    odd = (ELL[PAIR_FIRST] + ELL[PAIR_SECOND]) % 2 == 1
    factors = np.where(PAIR_FIRST == PAIR_SECOND, 1.0, 2.0)
    signs = np.stack([np.where(odd, 0.0, factors), np.where(odd, -factors, 0.0)], axis=1).astype(np.float32)
    angle = (np.outer(np.arange(NZ), np.arange(NZ)) % NZ) * (2.0 * np.pi / NZ)
    cos_z = np.cos(angle).reshape(NZ, groups, planes)
    sin_z = np.sin(angle).reshape(NZ, groups, planes)
    half = up(NZ, 128)
    spread = np.zeros((2 * half, groups, lanes), np.float32)
    spread[:NZ, :, :planes] = cos_z
    spread[half : half + NZ, :, :planes] = -sin_z
    spread[:NZ, :, planes : 2 * planes] = sin_z
    spread[half : half + NZ, :, planes : 2 * planes] = cos_z
    spread = spread.reshape(2 * half, groups * lanes)
    spread_high = spread.astype(BF16)
    spread_low = (spread - spread_high.astype(np.float32)).astype(BF16)
    vmem = pl.BlockSpec(memory_space=pltpu.VMEM)
    hbm = pl.BlockSpec(memory_space=pl.ANY)
    dma = pltpu.SemaphoreType.DMA
    part_lanes = up(NH * own, 128)
    received = pl.pallas_call(
        functools.partial(mega_kernel, bands, groups),
        in_specs=[vmem] * 6 + [pl.BlockSpec(memory_space=pltpu.SMEM), vmem, hbm, hbm],
        out_specs=vmem,
        out_shape=jax.ShapeDtypeStruct((devices, slots, lanes), F32),
        scratch_shapes=[
            pltpu.VMEM((8, atoms), F32),
            pltpu.VMEM((atoms, 8), F32),
            pltpu.VMEM((cols, 4 * width), BF16),
            pltpu.VMEM((HALF * block, 4 * width), BF16),
            pltpu.VMEM((steps, HALF, block, cols), F32),
            pltpu.VMEM((groups, HALF, own, cols), F32),
            pltpu.VMEM((points // tile, 2, atoms, tile), F32),
            pltpu.VMEM((up(HALF * own, 128), cols), F32),
            pltpu.VMEM((up(NH, 8), part_lanes), F32),
            pltpu.VMEM((bands, up(NH, 8), part_lanes), F32),
            pltpu.VMEM((chunk * chunks, own), F32),
            pltpu.VMEM((chunk, chunks * own), F32),
            pltpu.VMEM((groups, chunk, chunks * own), F32),
            pltpu.VMEM((up(SPECIES * pairs, 128), 2 * atoms), F32),
            pltpu.VMEM(aug_table.shape, BF16),
            pltpu.VMEM((2,) + spread.shape, BF16),
            pltpu.VMEM((8, points), F32),
            pltpu.VMEM((slots, 2 * half), F32),
            pltpu.VMEM((groups, slots, lanes), F32),
            dma((groups,)),
            dma((groups,)),
            dma((bands,)),
            dma((bands,)),
            dma((groups,)),
            dma((groups,)),
            dma((devices,)),
            dma((devices,)),
            dma((2,)),
        ],
        compiler_params=pltpu.CompilerParams(collective_id=0, has_side_effects=True),
        name="slots",
    )(
        waves,
        occupations[None, :],
        beta_table,
        wave_miller,
        atom_kinds[None, :],
        atom_sites,
        stick_columns,
        jnp.asarray(signs),
        aug_table,
        jnp.asarray(np.stack([spread_high, spread_low])),
    )
    y_block = NY // bands
    total = devices * slots
    batch = math.gcd(planes, 7)
    y_pad = up(y_block, 16)
    result = pl.pallas_call(
        functools.partial(finish_kernel, bands, planes),
        grid=(planes // batch,),
        in_specs=[pl.BlockSpec((total, lanes), lambda g: (0, 0))],
        out_specs=pl.BlockSpec((batch, y_block, 2, NX), lambda g: (g, 0, 0, 0)),
        out_shape=jax.ShapeDtypeStruct((planes, y_block, 2, NX), F32),
        scratch_shapes=[
            pltpu.VMEM((2, 2 * total, 512), BF16),
            pltpu.VMEM((lanes, total), F32),
            pltpu.VMEM((2, y_pad, total), F32),
            pltpu.VMEM((batch * y_pad, 2 * total), BF16),
        ],
        name="finish",
    )(received.reshape(total, lanes))
    return result.transpose(2, 0, 1, 3)


def solution(mesh):
    in_specs = (
        P(None, "band", "ga"),
        P("band"),
        P(None, "ga"),
        P(None, "ga"),
        P(),
        P(),
        P(None, ("band", "ga")),
        P(("band", "ga")),
    )
    out_specs = P(None, "ga", "band", None)
    return jax.shard_map(
        on_device, mesh=mesh, in_specs=in_specs, out_specs=out_specs, check_vma=False
    )
```
